8 devices in a mesh: dp: 1 (over z), tp: 2 (over y), sp: 4 (over x, core).
Axes of the slice: x: 2, y: 2, z: 1, core: 2. Of those that a mesh axis runs over, the one named last changes fastest.
Arguments:
- hidden: bfloat16 [16, 1024], P('dp')
- k_cache: bfloat16 [16, 16384, 16, 64], P('dp', 'sp', 'tp')
- v_cache: bfloat16 [16, 16384, 16, 64], P('dp', 'sp', 'tp')
- lengths: int32 [16], P('dp')
- rel_table: bfloat16 [16384, 16, 64], P('sp', 'tp')
- u_bias: bfloat16 [16, 64], P('tp')
- w_bias: bfloat16 [16, 64], P('tp')
- g_attn: bfloat16 [1024], replicated
- w_query: bfloat16 [1024, 16, 64], P(None, 'tp')
- w_key: bfloat16 [1024, 16, 64], P(None, 'tp')
- w_value: bfloat16 [1024, 16, 64], P(None, 'tp')
- w_out: bfloat16 [16, 64, 1024], P('tp')
- g_mlp: bfloat16 [1024], replicated
- w_up: bfloat16 [1024, 4096], P(None, 'tp')
- w_down: bfloat16 [4096, 1024], P('tp')
Outputs:
- output: bfloat16 [16, 1024], P('dp')
All inputs are finite; a program needn't handle non-finite values.
Results may differ from the reference program's by a relative error of at most 0.0166655.
Values sent between devices are 32-bit elements.
A program may use at most 1 GiB of HBM per device.

```python
import math
import jax
import jax.numpy as jnp
from jax import lax

BATCH = 16
SMAX = 16384
D = 1024
HEADS = 16
HEAD = 64
FF = 4096
EPS = 1e-6
MASKED = -1e30


def setup_inputs(seed: int = 0, part: int = 0) -> dict:
    base = jax.random.key(seed)
    shared_keys = jax.random.split(base, 11)
    part_keys = jax.random.split(jax.random.fold_in(base, part), 5)
    key_scale = math.sqrt(math.log(SMAX / 32.0) / 4.0)
    cache_shape = (BATCH, SMAX, HEADS, HEAD)
    hidden = jax.random.normal(part_keys[0], (BATCH, D), jnp.float32)
    k_cache = jax.random.normal(part_keys[1], cache_shape, jnp.float32) * key_scale
    v_cache = jax.random.normal(part_keys[2], cache_shape, jnp.float32)
    drawn_len = jax.random.randint(part_keys[3], (BATCH,), SMAX // 8, SMAX)
    full_slot = jax.random.randint(part_keys[4], (), 0, BATCH)
    lengths = jnp.where(jnp.arange(BATCH) == full_slot, SMAX - 1, drawn_len).astype(jnp.int32)
    rel_table = jax.random.normal(shared_keys[0], (SMAX, HEADS, HEAD), jnp.float32) * key_scale
    u_bias = jax.random.normal(shared_keys[1], (HEADS, HEAD), jnp.float32)
    w_bias = jax.random.normal(shared_keys[2], (HEADS, HEAD), jnp.float32)
    g_attn = 1.0 + 0.3 * jax.random.normal(shared_keys[3], (D,), jnp.float32)
    w_query = jax.random.normal(shared_keys[4], (D, HEADS, HEAD), jnp.float32) * D ** -0.5
    w_key = jax.random.normal(shared_keys[5], (D, HEADS, HEAD), jnp.float32) * (2.5 * key_scale * D ** -0.5)
    w_value = jax.random.normal(shared_keys[6], (D, HEADS, HEAD), jnp.float32) * (2.0 * D ** -0.5)
    w_out = jax.random.normal(shared_keys[7], (HEADS, HEAD, D), jnp.float32) * (3.0 * (HEADS * HEAD) ** -0.5)
    g_mlp = 1.0 + 0.3 * jax.random.normal(shared_keys[8], (D,), jnp.float32)
    w_up = jax.random.normal(shared_keys[9], (D, FF), jnp.float32) * D ** -0.5
    w_down = jax.random.normal(shared_keys[10], (FF, D), jnp.float32) * FF ** -0.5
    return {
        'hidden': hidden.astype(jnp.bfloat16),
        'k_cache': k_cache.astype(jnp.bfloat16),
        'v_cache': v_cache.astype(jnp.bfloat16),
        'lengths': lengths,
        'rel_table': rel_table.astype(jnp.bfloat16),
        'u_bias': u_bias.astype(jnp.bfloat16),
        'w_bias': w_bias.astype(jnp.bfloat16),
        'g_attn': g_attn.astype(jnp.bfloat16),
        'w_query': w_query.astype(jnp.bfloat16),
        'w_key': w_key.astype(jnp.bfloat16),
        'w_value': w_value.astype(jnp.bfloat16),
        'w_out': w_out.astype(jnp.bfloat16),
        'g_mlp': g_mlp.astype(jnp.bfloat16),
        'w_up': w_up.astype(jnp.bfloat16),
        'w_down': w_down.astype(jnp.bfloat16),
    }


def rms_norm(tensor, gain):
    wide = tensor.astype(jnp.float32)
    mean_sq = jnp.mean(wide * wide, axis=-1, keepdims=True)
    return (wide * lax.rsqrt(mean_sq + EPS) * gain.astype(jnp.float32)).astype(jnp.bfloat16)


def reference(hidden, k_cache, v_cache, lengths, rel_table, u_bias, w_bias, g_attn, w_query, w_key, w_value, w_out, g_mlp, w_up, w_down):
    normed = rms_norm(hidden, g_attn)
    query_vec = jnp.dot(normed, w_query.reshape(D, HEADS * HEAD), preferred_element_type=jnp.float32).astype(jnp.bfloat16).reshape(BATCH, HEADS, HEAD)
    key_new = jnp.dot(normed, w_key.reshape(D, HEADS * HEAD), preferred_element_type=jnp.float32).astype(jnp.bfloat16).reshape(BATCH, HEADS, HEAD)
    value_new = jnp.dot(normed, w_value.reshape(D, HEADS * HEAD), preferred_element_type=jnp.float32).astype(jnp.bfloat16).reshape(BATCH, HEADS, HEAD)
    positions = jnp.arange(SMAX)
    write_mask = (positions[None, :] == lengths[:, None])[:, :, None, None]
    k_updated = jnp.where(write_mask, key_new[:, None], k_cache)
    v_updated = jnp.where(write_mask, value_new[:, None], v_cache)
    q_content = (query_vec.astype(jnp.float32) + u_bias.astype(jnp.float32)).astype(jnp.bfloat16)
    q_position = (query_vec.astype(jnp.float32) + w_bias.astype(jnp.float32)).astype(jnp.bfloat16)
    rel_wide = rel_table.astype(jnp.float32)

    def attend_one(packed):
        q_cont, q_pos, k_seq, v_seq, length = packed
        content = jnp.einsum('hd,shd->hs', q_cont.astype(jnp.float32), k_seq.astype(jnp.float32))
        by_distance = jnp.einsum('hd,shd->hs', q_pos.astype(jnp.float32), rel_wide)
        distance = length - positions
        relative = by_distance[:, jnp.clip(distance, 0, SMAX - 1)]
        scores = (content + relative) * (HEAD ** -0.5)
        scores = jnp.where((distance >= 0)[None, :], scores, MASKED)
        weights = jax.nn.softmax(scores, axis=-1)
        return jnp.einsum('hs,shd->hd', weights, v_seq.astype(jnp.float32)).astype(jnp.bfloat16)

    context = lax.map(attend_one, (q_content, q_position, k_updated, v_updated, lengths))
    attn_out = jnp.dot(context.reshape(BATCH, HEADS * HEAD), w_out.reshape(HEADS * HEAD, D), preferred_element_type=jnp.float32)
    resid_mid = (hidden.astype(jnp.float32) + attn_out).astype(jnp.bfloat16)
    normed_mlp = rms_norm(resid_mid, g_mlp)
    up_proj = jnp.dot(normed_mlp, w_up, preferred_element_type=jnp.float32)
    activated = jax.nn.gelu(up_proj, approximate=True).astype(jnp.bfloat16)
    down_proj = jnp.dot(activated, w_down, preferred_element_type=jnp.float32)
    hidden_out = (resid_mid.astype(jnp.float32) + down_proj).astype(jnp.bfloat16)
    return hidden_out
```

```python
import functools

import jax
import jax.numpy as jnp
from jax import lax
from jax.experimental import pallas as pl
from jax.experimental.pallas import tpu as pltpu
from jax.sharding import PartitionSpec as P

EPS = 1e-6
MASKED = -1e30
MESH = pl.DeviceIdType.MESH
F32 = jnp.float32
BF16 = jnp.bfloat16
NT = (((1,), (1,)), ((), ()))
NS = 10


def rms(x, gain):
    mean_sq = jnp.mean(x * x, axis=-1, keepdims=True)
    return (x * lax.rsqrt(mean_sq + EPS) * gain).astype(BF16)


def kernel(hid_ref, k_hbm, v_hbm, len_ref, r_hbm, u_ref, w_ref, ga_ref, wq_hbm, wk_hbm, wv_hbm, wo_hbm, gm_ref, wu_hbm, wd_hbm,
           out_ref,
           ring, rel_own, rel_par, rel_cro, rel_dia, content, wo, wu, wd, qc_bd, k_new, v_new, rows_acc, part, asend, arecv, dsend, drecv,
           ring_sem, wt_sem, par_sem, cro_send, cro_recv, dia_send, dia_recv, part_send, part_recv, ex_sem):
    nb, nh, width = content.shape
    feat = k_hbm.shape[1]
    hd = feat // nh
    sp = lax.axis_index("sp")
    tp = lax.axis_index("tp")
    chip = sp // 2
    core = lax.rem(sp, 2)
    partner = chip * 2 + (1 - core)
    cross = (1 - chip) * 2 + core
    diag = (1 - chip) * 2 + (1 - core)

    barrier = pltpu.get_barrier_semaphore()
    for peer in (partner, cross, diag):
        pl.semaphore_signal(barrier, inc=1, device_id={"sp": peer}, device_id_type=MESH)
    pl.semaphore_signal(barrier, inc=1, device_id={"tp": 1 - tp}, device_id_type=MESH)

    def load(src, dst, sem):
        return pltpu.make_async_copy(src, dst, sem)

    def k_load(b):
        return load(k_hbm.at[b], ring.at[lax.rem(b, NS)], ring_sem.at[lax.rem(b, NS)])

    def v_load(b):
        slot = lax.rem(b + nb, NS)
        return load(v_hbm.at[b], ring.at[slot], ring_sem.at[slot])

    wdt = wq_hbm.shape[1]
    stage = ring.at[NS - 2]
    r_copy = load(r_hbm, ring.at[NS - 1], ring_sem.at[NS - 1])
    wq_copy = load(wq_hbm, stage.at[:, pl.ds(0, wdt)], wt_sem.at[0])
    wk_copy = load(wk_hbm, stage.at[:, pl.ds(wdt, wdt)], wt_sem.at[1])
    wv_copy = load(wv_hbm, stage.at[:, pl.ds(2 * wdt, wdt)], wt_sem.at[2])
    wo_copy = load(wo_hbm, wo, wt_sem.at[3])
    wu_copy = load(wu_hbm, wu, wt_sem.at[4])
    wd_copy = load(wd_hbm, wd, wt_sem.at[5])
    wq_copy.start()
    r_copy.start()
    wk_copy.start()
    wv_copy.start()
    for b in range(NS - 2):
        k_load(b).start()

    hidden = hid_ref[...].astype(F32)
    normed = rms(hidden, ga_ref[...].astype(F32))

    head_of_row = lax.broadcasted_iota(jnp.int32, (nh, feat), 0)
    head_of_col = lax.broadcasted_iota(jnp.int32, (nh, feat), 1) // hd
    diag_mask = head_of_row == head_of_col
    spread_row = lax.broadcasted_iota(jnp.int32, (hd, feat), 0)
    spread_col = lax.rem(lax.broadcasted_iota(jnp.int32, (hd, feat), 1), hd)
    spread = (spread_row == spread_col).astype(BF16)
    u_wide = jnp.dot(u_ref[...], spread, preferred_element_type=F32)
    w_wide = jnp.dot(w_ref[...], spread, preferred_element_type=F32)

    wq_copy.wait()
    query = lax.dot_general(normed, stage[:, pl.ds(0, wdt)], NT, preferred_element_type=F32).astype(BF16).astype(F32)
    zero_rows = jnp.zeros((nh, feat), F32)
    pos_rows = []
    for b in range(nb):
        row = query[b:b + 1, :]
        qc = jnp.where(diag_mask, row + u_wide, 0.0)
        qc_bd[b] = jnp.concatenate([qc, zero_rows], axis=0).astype(BF16)
        pos_rows.append(jnp.where(diag_mask, row + w_wide, 0.0))
    q_pos = jnp.concatenate(pos_rows, axis=0).astype(BF16)

    r_copy.wait()
    step = 1024
    for c in range(width // step):
        cols = pl.ds(c * step, step)
        prod = jnp.dot(q_pos, ring[NS - 1, :, cols], preferred_element_type=F32)
        rel_own[:, :, cols] = prod.reshape(nb, nh, step)
    pl.semaphore_wait(barrier, 4)

    par_copy = pltpu.make_async_remote_copy(src_ref=rel_own, dst_ref=rel_par, send_sem=par_sem.at[0], recv_sem=par_sem.at[1],
                                            device_id={"sp": partner}, device_id_type=MESH)

    def cross_copy(i):
        return pltpu.make_async_remote_copy(src_ref=rel_own.at[i], dst_ref=rel_cro.at[i], send_sem=cro_send.at[i], recv_sem=cro_recv.at[i],
                                            device_id={"sp": cross}, device_id_type=MESH)

    def forward_copy(i):
        return pltpu.make_async_remote_copy(src_ref=rel_cro.at[i], dst_ref=rel_dia.at[i], send_sem=dia_send.at[i], recv_sem=dia_recv.at[i],
                                            device_id={"sp": partner}, device_id_type=MESH)

    par_copy.start()
    for i in range(nb):
        cross_copy(i).start()

    wk_copy.wait()
    k_new[...] = lax.dot_general(normed, stage[:, pl.ds(wdt, wdt)], NT, preferred_element_type=F32).astype(BF16).astype(F32)
    wv_copy.wait()
    v_new[...] = lax.dot_general(normed, stage[:, pl.ds(2 * wdt, wdt)], NT, preferred_element_type=F32).astype(BF16).astype(F32)
    for b in range(NS - 2, NS):
        k_load(b).start()

    @pl.loop(0, nb)
    def _(b):
        k_load(b).wait()
        content[b] = jnp.dot(qc_bd[b], ring[lax.rem(b, NS)], preferred_element_type=F32)[:nh]

        @pl.when(b < nb - NS)
        def _():
            k_load(b + NS).start()

        @pl.when(b >= nb - NS)
        def _():
            v_load(b + NS - nb).start()

    wo_copy.start()
    wu_copy.start()
    wd_copy.start()
    par_copy.wait()

    lane = lax.broadcasted_iota(jnp.int32, (nh, width), 1)
    back = 127 - lax.broadcasted_iota(jnp.int32, (nh, 128), 1)
    stat_lane = lax.broadcasted_iota(jnp.int32, (nh, 128), 1)
    stat_row = lax.broadcasted_iota(jnp.int32, (nh, 128), 0)

    def attend(b):
        length = len_ref[b]
        high = length // width
        low = length - high * width
        first = high - sp
        upper = lane <= low
        comb = jnp.zeros((nh, width), F32)
        for block, rows in ((sp, rel_own), (partner, rel_par), (cross, rel_cro), (diag, rel_dia)):
            want = jnp.where(upper, first, first - 1) == block
            comb = jnp.where(want, rows[b], comb)
        pieces = [jnp.take_along_axis(comb[:, 128 * c:128 * c + 128], back, axis=1) for c in range(width // 128)]
        relative = pltpu.roll(jnp.concatenate(pieces[::-1], axis=1), lax.rem(low + 1, width), axis=1)
        here = length - sp * width
        valid = lane <= here
        is_new = lane == here
        q_rows = qc_bd[b][:nh].astype(F32)
        s_new = jnp.sum(q_rows * k_new[pl.ds(b, 1), :], axis=1, keepdims=True)
        scores = jnp.where(is_new, s_new, content[b]) + relative
        scores = jnp.where(valid, scores * (hd ** -0.5), MASKED)
        top = jnp.max(scores, axis=1, keepdims=True)
        weights = jnp.where(valid, jnp.exp(scores - top), 0.0)
        total = jnp.sum(weights, axis=1, keepdims=True)
        p_new = jnp.sum(jnp.where(is_new, weights, 0.0), axis=1, keepdims=True).astype(BF16).astype(F32)
        cached = jnp.where(is_new, 0.0, weights).astype(BF16)
        slot = lax.rem(b + nb, NS)
        v_load(b).wait()
        mixed = lax.dot_general(cached, ring[slot], NT, preferred_element_type=F32)
        mixed = mixed + p_new * v_new[pl.ds(b, 1), :]
        rows_acc[b, :, pl.ds(0, feat)] = jnp.sum(jnp.where(diag_mask, mixed, 0.0), axis=0, keepdims=True)
        stats = jnp.where(stat_lane == stat_row, top, jnp.where(stat_lane == stat_row + nh, total, 0.0))
        rows_acc[b, :, pl.ds(feat, 128)] = jnp.sum(stats, axis=0, keepdims=True)

        @pl.when(b < nb - NS)
        def _():
            v_load(b + NS).start()

    @pl.loop(0, nb + 1)
    def _(i):
        @pl.when(i < nb)
        def _():
            cross_copy(i).wait()
            forward_copy(i).start()

        @pl.when(i >= 1)
        def _():
            forward_copy(i - 1).wait()
            attend(i - 1)

    for b in range(nb):
        part[0, b:b + 1, :] = rows_acc[b]
    part_copies = []
    for j, peer in ((1, partner), (2, cross), (3, diag)):
        part_copies.append(pltpu.make_async_remote_copy(src_ref=part.at[0], dst_ref=part.at[j], send_sem=part_send.at[j], recv_sem=part_recv.at[j],
                                                        device_id={"sp": peer}, device_id_type=MESH))
    for copy in part_copies:
        copy.start()
    for copy in part_copies:
        copy.wait()

    blocks = []
    for s in range(4):
        j = lax.rem(chip + s // 2, 2) * 2 + lax.rem(core + s % 2, 2)
        blocks.append(part[j])
    tops = [x[:, feat:] for x in blocks]
    top_all = functools.reduce(jnp.maximum, tops)
    scale = [jnp.exp(t - top_all) for t in tops]
    total = sum(s * pltpu.roll(t, 128 - nh, axis=1) for s, t in zip(scale, tops))
    lane_head = lax.broadcasted_iota(jnp.int32, (nb, 128), 1) // hd
    context = jnp.zeros((nb, feat), F32)
    for s, x in zip(scale, blocks):
        factor = s / total
        wide = jnp.concatenate([jnp.take_along_axis(factor, lane_head + c * (128 // hd), axis=1) for c in range(feat // 128)], axis=1)
        context = context + wide * x[:, :feat]

    def exchange(send, recv, j):
        return pltpu.make_async_remote_copy(src_ref=send, dst_ref=recv, send_sem=ex_sem.at[2 * j], recv_sem=ex_sem.at[2 * j + 1],
                                            device_id={"tp": 1 - tp}, device_id_type=MESH)

    wo_copy.wait()
    attn = jnp.dot(context.astype(BF16), wo[...], preferred_element_type=F32)
    asend[...] = attn
    swap = exchange(asend, arecv, 0)
    swap.start()
    swap.wait()
    middle = (hidden + (attn + arecv[...])).astype(BF16).astype(F32)
    normed_mlp = rms(middle, gm_ref[...].astype(F32))
    wu_copy.wait()
    up = jnp.dot(normed_mlp, wu[...], preferred_element_type=F32)
    act = jax.nn.gelu(up, approximate=True).astype(BF16)
    wd_copy.wait()
    down = jnp.dot(act, wd[...], preferred_element_type=F32)
    dsend[...] = down
    swap = exchange(dsend, drecv, 1)
    swap.start()
    swap.wait()
    out_ref[...] = (middle + (down + drecv[...])).astype(BF16)


def solution(mesh):
    spec_cache = P('dp', 'sp', 'tp', None)
    in_specs = (P('dp', None), spec_cache, spec_cache, P('dp'), P('sp', 'tp', None), P('tp', None), P('tp', None), P(None), P(None, 'tp', None), P(None, 'tp', None), P(None, 'tp', None), P('tp', None, None), P(None), P(None, 'tp'), P('tp', None))

    def layer_step(hidden, k_cache, v_cache, lengths, rel_table, u_bias, w_bias, g_attn, w_query, w_key, w_value, w_out, g_mlp, w_up, w_down):
        nb, width, nh, hd = k_cache.shape
        feat = nh * hd
        model = hidden.shape[1]
        k_t = k_cache.transpose(0, 2, 3, 1).reshape(nb, feat, width)
        v_t = v_cache.transpose(0, 2, 3, 1).reshape(nb, feat, width)
        r_t = rel_table.transpose(1, 2, 0).reshape(feat, width)
        proj = [w.transpose(1, 2, 0).reshape(feat, model) for w in (w_query, w_key, w_value)]
        vmem = pl.BlockSpec(memory_space=pltpu.VMEM)
        hbm = pl.BlockSpec(memory_space=pl.ANY)
        smem = pl.BlockSpec(memory_space=pltpu.SMEM)
        dma = pltpu.SemaphoreType.DMA
        return pl.pallas_call(
            kernel,
            out_shape=jax.ShapeDtypeStruct((nb, model), BF16),
            in_specs=[vmem, hbm, hbm, smem, hbm, vmem, vmem, vmem, hbm, hbm, hbm, hbm, vmem, hbm, hbm],
            out_specs=vmem,
            scratch_shapes=[
                pltpu.VMEM((NS, feat, width), BF16),
                pltpu.VMEM((nb, nh, width), F32),
                pltpu.VMEM((nb, nh, width), F32),
                pltpu.VMEM((nb, nh, width), F32),
                pltpu.VMEM((nb, nh, width), F32),
                pltpu.VMEM((nb, nh, width), F32),
                pltpu.VMEM((feat, model), BF16),
                pltpu.VMEM(w_up.shape, BF16),
                pltpu.VMEM(w_down.shape, BF16),
                pltpu.VMEM((nb, 16, feat), BF16),
                pltpu.VMEM((nb, feat), F32),
                pltpu.VMEM((nb, feat), F32),
                pltpu.VMEM((nb, 1, feat + 128), F32),
                pltpu.VMEM((4, nb, feat + 128), F32),
                pltpu.VMEM((nb, model), F32),
                pltpu.VMEM((nb, model), F32),
                pltpu.VMEM((nb, model), F32),
                pltpu.VMEM((nb, model), F32),
                dma((NS,)), dma((6,)), dma((2,)), dma((nb,)), dma((nb,)), dma((nb,)), dma((nb,)), dma((4,)), dma((4,)), dma((4,)),
            ],
            compiler_params=pltpu.CompilerParams(collective_id=0, has_side_effects=True, vmem_limit_bytes=67043328),
        )(hidden, k_t, v_t, lengths, r_t, u_bias, w_bias, g_attn[None], *proj, w_out.reshape(feat, model), g_mlp[None], w_up, w_down)

    return jax.shard_map(layer_step, mesh=mesh, in_specs=in_specs, out_specs=P('dp', None), check_vma=False)
```

```python
import functools

import jax
import jax.numpy as jnp
from jax import lax
from jax.experimental import pallas as pl
from jax.experimental.pallas import tpu as pltpu
from jax.sharding import PartitionSpec as P

EPS = 1e-6
MASKED = -1e30
MESH = pl.DeviceIdType.MESH
F32 = jnp.float32
BF16 = jnp.bfloat16
NT = (((1,), (1,)), ((), ()))
NS = 10
GROUP = 4
STAGES = 4


def rms(x, gain):
    mean_sq = jnp.mean(x * x, axis=-1, keepdims=True)
    return (x * lax.rsqrt(mean_sq + EPS) * gain).astype(BF16)


def kernel(caps, hid_hbm, k_hbm, v_hbm, len_hbm, r_hbm, u_hbm, w_hbm, ga_hbm, wq_hbm, wk_hbm, wv_hbm, wo_hbm, gm_hbm, wu_hbm, wd_hbm,
           out_ref,
           hid_ref, len_ref, u_ref, w_ref, ga_ref, gm_ref, ring, rel_own, rel_par, content, probs, p_extra, wo, wu, wd, qc_bd, k_new, v_new, rows_acc, part, asend, arecv, dsend, drecv,
           ring_sem, wt_sem, r_sem, par_sem, cro_send, cro_recv, dia_send, dia_recv, part_send, part_recv, ex_sem, table, *far_refs):
    nb, nh, width = content.shape
    feat = k_hbm.shape[1]
    hd = feat // nh
    even, odd = caps
    compact = even[-1] < nb
    rel_cro, rel_dia = far_refs[:STAGES], far_refs[STAGES:2 * STAGES]
    rel_send = far_refs[-1] if compact else rel_own
    sp = lax.axis_index("sp")
    tp = lax.axis_index("tp")
    chip = sp // 2
    core = lax.rem(sp, 2)
    partner = chip * 2 + (1 - core)
    cross = (1 - chip) * 2 + core
    diag = (1 - chip) * 2 + (1 - core)

    def by_core(c, a, b):
        return a + (b - a) * c

    def size(g, c):
        return by_core(c, even[g + 1] - even[g], odd[g + 1] - odd[g])

    def begin(g, c):
        return by_core(c, even[g], odd[g])

    barrier = pltpu.get_barrier_semaphore()
    for peer in (partner, cross, diag):
        pl.semaphore_signal(barrier, inc=1, device_id={"sp": peer}, device_id_type=MESH)
    pl.semaphore_signal(barrier, inc=1, device_id={"tp": 1 - tp}, device_id_type=MESH)

    def load(src, dst, sem):
        return pltpu.make_async_copy(src, dst, sem)

    def k_load(b):
        return load(k_hbm.at[b], ring.at[lax.rem(b, NS)], ring_sem.at[lax.rem(b, NS)])

    def v_load(b):
        slot = lax.rem(b + nb, NS)
        return load(v_hbm.at[b], ring.at[slot], ring_sem.at[slot])

    small = [load(a, b, wt_sem.at[6 + i]) for i, (a, b) in enumerate(((hid_hbm, hid_ref), (ga_hbm, ga_ref), (len_hbm, len_ref), (u_hbm, u_ref), (w_hbm, w_ref), (gm_hbm, gm_ref)))]
    for copy in small:
        copy.start()
    wdt = wq_hbm.shape[1]
    stage = ring.at[NS - 2]
    step = 1024
    r_copies = [load(r_hbm.at[:, pl.ds(c, step)], ring.at[NS - 1, :, pl.ds(c, step)], r_sem.at[c // step]) for c in range(0, width, step)]
    wq_copy = load(wq_hbm, stage.at[:, pl.ds(0, wdt)], wt_sem.at[0])
    wk_copy = load(wk_hbm, stage.at[:, pl.ds(wdt, wdt)], wt_sem.at[1])
    wv_copy = load(wv_hbm, stage.at[:, pl.ds(2 * wdt, wdt)], wt_sem.at[2])
    wo_copy = load(wo_hbm, wo, wt_sem.at[3])
    wu_copy = load(wu_hbm, wu, wt_sem.at[4])
    wd_copy = load(wd_hbm, wd, wt_sem.at[5])
    wq_copy.start()
    for copy in r_copies:
        copy.start()
    wk_copy.start()
    wv_copy.start()
    for b in range(NS - 2):
        k_load(b).start()

    for copy in small:
        copy.wait()
    if compact:
        for level in range(2):
            rank = jnp.int32(0)
            for b in range(nb):
                table[level, b] = rank
                rank = rank + (len_ref[b] >= (2 + level) * width).astype(jnp.int32)
        reach = [len_ref[b] >= (2 + core) * width for b in range(nb)]
        ranks = [table[core, b] for b in range(nb)]
        chosen = {}
        for g in range(STAGES):
            for c in range(even[g + 1] - even[g]):
                want = begin(g, core) + c
                chosen[g, c] = functools.reduce(jnp.add, [jnp.where(reach[b] & (ranks[b] == want), b, 0) for b in range(nb)])

    hidden = hid_ref[...].astype(F32)
    normed = rms(hidden, ga_ref[...][None].astype(F32))

    head_of_row = lax.broadcasted_iota(jnp.int32, (nh, feat), 0)
    head_of_col = lax.broadcasted_iota(jnp.int32, (nh, feat), 1) // hd
    diag_mask = head_of_row == head_of_col
    spread_row = lax.broadcasted_iota(jnp.int32, (hd, feat), 0)
    spread_col = lax.rem(lax.broadcasted_iota(jnp.int32, (hd, feat), 1), hd)
    spread = (spread_row == spread_col).astype(BF16)
    u_wide = jnp.dot(u_ref[...], spread, preferred_element_type=F32)
    w_wide = jnp.dot(w_ref[...], spread, preferred_element_type=F32)

    wq_copy.wait()
    query = lax.dot_general(normed, stage[:, pl.ds(0, wdt)], NT, preferred_element_type=F32).astype(BF16).astype(F32)
    zero_rows = jnp.zeros((nh, feat), F32)
    pos_rows = []
    for b in range(nb):
        row = query[b:b + 1, :]
        qc = jnp.where(diag_mask, row + u_wide, 0.0)
        qc_bd[b] = jnp.concatenate([qc, zero_rows], axis=0).astype(BF16)
        pos_rows.append(jnp.where(diag_mask, row + w_wide, 0.0))
    q_pos = jnp.concatenate(pos_rows, axis=0).astype(BF16)

    for c in range(width // step):
        cols = pl.ds(c * step, step)
        r_copies[c].wait()
        prod = jnp.dot(q_pos, ring[NS - 1, :, cols], preferred_element_type=F32)
        rel_own[:, :, cols] = prod.reshape(nb, nh, step)
    pl.semaphore_wait(barrier, 4)

    par_copy = pltpu.make_async_remote_copy(src_ref=rel_own, dst_ref=rel_par, send_sem=par_sem.at[0], recv_sem=par_sem.at[1],
                                            device_id={"sp": partner}, device_id_type=MESH)

    def cross_copy(g, c):
        i = even[g] + c
        return pltpu.make_async_remote_copy(src_ref=rel_send.at[i], dst_ref=rel_cro[g].at[c], send_sem=cro_send.at[i], recv_sem=cro_recv.at[i],
                                            device_id={"sp": cross}, device_id_type=MESH)

    def forward_copy(g, c):
        i = even[g] + c
        return pltpu.make_async_remote_copy(src_ref=rel_cro[g].at[c], dst_ref=rel_dia[g].at[c], send_sem=dia_send.at[i], recv_sem=dia_recv.at[i],
                                            device_id={"sp": partner}, device_id_type=MESH)

    for g in range(STAGES):
        for c in range(even[g + 1] - even[g]):
            if compact:
                rel_send[even[g] + c] = rel_own[chosen[g, c]]

            @pl.when(c < size(g, core))
            def _():
                cross_copy(g, c).start()
        if g == 0:
            par_copy.start()

    wk_copy.wait()
    k_new[...] = lax.dot_general(normed, stage[:, pl.ds(wdt, wdt)], NT, preferred_element_type=F32).astype(BF16).astype(F32)
    wv_copy.wait()
    v_new[...] = lax.dot_general(normed, stage[:, pl.ds(2 * wdt, wdt)], NT, preferred_element_type=F32).astype(BF16).astype(F32)
    for b in range(NS - 2, NS):
        k_load(b).start()

    def arrive(g, c):
        @pl.when((c >= 0) & (c < size(g, core)))
        def _():
            cross_copy(g, c).wait()
            forward_copy(g, c).start()

    @pl.loop(0, nb)
    def _(b):
        @pl.when(b == nb - 3)
        def _():
            for c in range(rel_cro[0].shape[0]):
                arrive(0, c)

        k_load(b).wait()
        content[b] = jnp.dot(qc_bd[b], ring[lax.rem(b, NS)], preferred_element_type=F32)[:nh]

        @pl.when(b < nb - NS)
        def _():
            k_load(b + NS).start()

        @pl.when(b >= nb - NS)
        def _():
            v_load(b + NS - nb).start()

    par_copy.wait()

    lane = lax.broadcasted_iota(jnp.int32, (nh, width), 1)
    back = 127 - lax.broadcasted_iota(jnp.int32, (nh, 128), 1)
    stat_lane = lax.broadcasted_iota(jnp.int32, (nh, 128), 1)
    stat_row = lax.broadcasted_iota(jnp.int32, (nh, 128), 0)

    def pick(rows, g, b, level):
        if not compact:
            return rows[g][b - g * GROUP]
        unit = table[level, b]
        x = rows[0][jnp.minimum(unit, rows[0].shape[0] - 1)]
        for h in range(1, g + 1):
            local = unit - begin(h, level)
            x = jnp.where(local >= 0, rows[h][jnp.clip(local, 0, rows[h].shape[0] - 1)], x)
        return x

    def score(g, b, slot):
        length = len_ref[b]
        high = length // width
        low = length - high * width
        first = high - sp
        upper = lane <= low
        far = pick(rel_cro, g, b, core)
        farther = pick(rel_dia, g, b, 1 - core)
        comb = jnp.zeros((nh, width), F32)
        for block, rows in ((sp, rel_own[b]), (partner, rel_par[b]), (cross, far), (diag, farther)):
            want = jnp.where(upper, first, first - 1) == block
            comb = jnp.where(want, rows, comb)
        pieces = [jnp.take_along_axis(comb[:, 128 * c:128 * c + 128], back, axis=1) for c in range(width // 128)]
        relative = pltpu.roll(jnp.concatenate(pieces[::-1], axis=1), lax.rem(low + 1, width), axis=1)
        here = length - sp * width
        valid = lane <= here
        is_new = lane == here
        q_rows = qc_bd[b][:nh].astype(F32)
        s_new = jnp.sum(q_rows * k_new[pl.ds(b, 1), :], axis=1, keepdims=True)
        scores = jnp.where(is_new, s_new, content[b]) + relative
        scores = jnp.where(valid, scores * (hd ** -0.5), MASKED)
        top = jnp.max(scores, axis=1, keepdims=True)
        weights = jnp.where(valid, jnp.exp(scores - top), 0.0)
        total = jnp.sum(weights, axis=1, keepdims=True)
        p_new = jnp.sum(jnp.where(is_new, weights, 0.0), axis=1, keepdims=True).astype(BF16).astype(F32)
        probs[slot] = jnp.where(is_new, 0.0, weights).astype(BF16)
        p_extra[slot] = jnp.broadcast_to(p_new, (nh, 128))
        stats = jnp.where(stat_lane == stat_row, top, jnp.where(stat_lane == stat_row + nh, total, 0.0))
        rows_acc[b, :, pl.ds(feat, 128)] = jnp.sum(stats, axis=0, keepdims=True)

    def mix(b, slot):
        mixed = lax.dot_general(probs[slot], ring[lax.rem(b + nb, NS)], NT, preferred_element_type=F32)
        mixed = mixed + p_extra[slot][:, :1] * v_new[pl.ds(b, 1), :]
        rows_acc[b, :, pl.ds(0, feat)] = jnp.sum(jnp.where(diag_mask, mixed, 0.0), axis=0, keepdims=True)

    def settle(g):
        for c in range(rel_cro[g].shape[0]):
            @pl.when(c < size(g, core))
            def _():
                forward_copy(g, c).wait_send()

            @pl.when(c < size(g, 1 - core))
            def _():
                forward_copy(g, c).wait_recv()

    settle(0)
    score(0, 0, 0)

    for g in range(nb // GROUP):
        late = rel_cro[g + 1].shape[0] if g + 1 < STAGES else 0
        first_step = max(g * GROUP - 1, 0)
        last_step = g * GROUP + GROUP - 2
        if g > 0:
            settle(g)
        for c in range(late - (last_step - first_step + 1)):
            arrive(g + 1, c)

        @pl.loop(first_step, last_step + 1)
        def _(i):
            if late:
                arrive(g + 1, i - last_step + late - 1)

            v_load(i).wait()
            mix(i, lax.rem(i, 2))
            score(g, i + 1, lax.rem(i + 1, 2))

            @pl.when(i < nb - NS)
            def _():
                v_load(i + NS).start()

    wo_copy.start()
    wu_copy.start()
    wd_copy.start()
    v_load(nb - 1).wait()
    mix(nb - 1, (nb - 1) % 2)

    for b in range(nb):
        part[0, b:b + 1, :] = rows_acc[b]
    part_copies = []
    for j, peer in ((1, partner), (2, cross), (3, diag)):
        part_copies.append(pltpu.make_async_remote_copy(src_ref=part.at[0], dst_ref=part.at[j], send_sem=part_send.at[j], recv_sem=part_recv.at[j],
                                                        device_id={"sp": peer}, device_id_type=MESH))
    for copy in part_copies:
        copy.start()
    for copy in part_copies:
        copy.wait()

    blocks = []
    for s in range(4):
        j = lax.rem(chip + s // 2, 2) * 2 + lax.rem(core + s % 2, 2)
        blocks.append(part[j])
    tops = [x[:, feat:] for x in blocks]
    top_all = functools.reduce(jnp.maximum, tops)
    scale = [jnp.exp(t - top_all) for t in tops]
    total = sum(s * pltpu.roll(t, 128 - nh, axis=1) for s, t in zip(scale, tops))
    lane_head = lax.broadcasted_iota(jnp.int32, (nb, 128), 1) // hd
    context = jnp.zeros((nb, feat), F32)
    for s, x in zip(scale, blocks):
        factor = s / total
        wide = jnp.concatenate([jnp.take_along_axis(factor, lane_head + c * (128 // hd), axis=1) for c in range(feat // 128)], axis=1)
        context = context + wide * x[:, :feat]

    def exchange(send, recv, j):
        return pltpu.make_async_remote_copy(src_ref=send, dst_ref=recv, send_sem=ex_sem.at[2 * j], recv_sem=ex_sem.at[2 * j + 1],
                                            device_id={"tp": 1 - tp}, device_id_type=MESH)

    wo_copy.wait()
    attn = jnp.dot(context.astype(BF16), wo[...], preferred_element_type=F32)
    asend[...] = attn
    swap = exchange(asend, arecv, 0)
    swap.start()
    swap.wait()
    middle = (hidden + (attn + arecv[...])).astype(BF16).astype(F32)
    normed_mlp = rms(middle, gm_ref[...][None].astype(F32))
    wu_copy.wait()
    up = jnp.dot(normed_mlp, wu[...], preferred_element_type=F32)
    act = jax.nn.gelu(up, approximate=True).astype(BF16)
    wd_copy.wait()
    down = jnp.dot(act, wd[...], preferred_element_type=F32)
    dsend[...] = down
    swap = exchange(dsend, drecv, 1)
    swap.start()
    swap.wait()
    out_ref[...] = (middle + (down + drecv[...])).astype(BF16)


def solution(mesh):
    spec_cache = P('dp', 'sp', 'tp', None)
    in_specs = (P('dp', None), spec_cache, spec_cache, P('dp'), P('sp', 'tp', None), P('tp', None), P('tp', None), P(None), P(None, 'tp', None), P(None, 'tp', None), P(None, 'tp', None), P('tp', None, None), P(None), P(None, 'tp'), P('tp', None))

    def layer_step(hidden, k_cache, v_cache, lengths, rel_table, u_bias, w_bias, g_attn, w_query, w_key, w_value, w_out, g_mlp, w_up, w_down):
        nb, width, nh, hd = k_cache.shape
        feat = nh * hd
        model = hidden.shape[1]
        k_t = k_cache.transpose(0, 2, 3, 1).reshape(nb, feat, width)
        v_t = v_cache.transpose(0, 2, 3, 1).reshape(nb, feat, width)
        r_t = rel_table.transpose(1, 2, 0).reshape(feat, width)
        proj = [w.transpose(1, 2, 0).reshape(feat, model) for w in (w_query, w_key, w_value)]
        vmem = pl.BlockSpec(memory_space=pltpu.VMEM)
        hbm = pl.BlockSpec(memory_space=pl.ANY)
        dma = pltpu.SemaphoreType.DMA
        full = 2 * (tuple(range(0, nb + 1, nb // STAGES)),)
        tight = (0, 4, 7, 10, 13), (0, 3, 5, 7, 8)

        def call(caps, *operands):
            compact = caps != full
            rows = caps[0][-1]
            return pl.pallas_call(
                functools.partial(kernel, caps),
                out_shape=jax.ShapeDtypeStruct((nb, model), BF16),
                in_specs=15 * [hbm],
                out_specs=vmem,
                scratch_shapes=[
                    pltpu.VMEM(hidden.shape, BF16),
                    pltpu.SMEM(lengths.shape, jnp.int32),
                    pltpu.VMEM(u_bias.shape, BF16),
                    pltpu.VMEM(w_bias.shape, BF16),
                    pltpu.VMEM(g_attn.shape, BF16),
                    pltpu.VMEM(g_mlp.shape, BF16),
                    pltpu.VMEM((NS, feat, width), BF16),
                    pltpu.VMEM((nb, nh, width), F32),
                    pltpu.VMEM((nb, nh, width), F32),
                    pltpu.VMEM((nb, nh, width), F32),
                    pltpu.VMEM((2, nh, width), BF16),
                    pltpu.VMEM((2, nh, 128), F32),
                    pltpu.VMEM((feat, model), BF16),
                    pltpu.VMEM(w_up.shape, BF16),
                    pltpu.VMEM(w_down.shape, BF16),
                    pltpu.VMEM((nb, 16, feat), BF16),
                    pltpu.VMEM((nb, feat), F32),
                    pltpu.VMEM((nb, feat), F32),
                    pltpu.VMEM((nb, 1, feat + 128), F32),
                    pltpu.VMEM((4, nb, feat + 128), F32),
                    pltpu.VMEM((nb, model), F32),
                    pltpu.VMEM((nb, model), F32),
                    pltpu.VMEM((nb, model), F32),
                    pltpu.VMEM((nb, model), F32),
                    dma((NS,)), dma((12,)), dma((4,)), dma((2,)), dma((rows,)), dma((rows,)), dma((rows,)), dma((rows,)), dma((4,)), dma((4,)), dma((4,)),
                    pltpu.SMEM((2, nb), jnp.int32),
                ] + 2 * [pltpu.VMEM((b - a, nh, width), F32) for a, b in zip(caps[0], caps[0][1:])] + ([pltpu.VMEM((rows, nh, width), F32)] if compact else []),
                compiler_params=pltpu.CompilerParams(collective_id=int(compact), has_side_effects=True, vmem_limit_bytes=67043328),
            )(*operands)

        operands = (hidden, k_t, v_t, lengths, r_t, u_bias, w_bias, g_attn, *proj, w_out.reshape(feat, model), g_mlp, w_up, w_down)
        seen = jnp.arange(nb)[:, None] < jnp.arange(nb // STAGES, nb + 1, nb // STAGES)[None]
        counts = [jnp.sum(jnp.where((lengths >= level * width)[:, None] & seen, 1, 0), axis=0) for level in (2, 3)]
        fits = functools.reduce(jnp.logical_and, [jnp.all(n <= jnp.array(cap[1:])) for n, cap in zip(counts, tight)])
        return lax.cond(fits, functools.partial(call, tight), functools.partial(call, full), *operands)

    return jax.shard_map(layer_step, mesh=mesh, in_specs=in_specs, out_specs=P('dp', None), check_vma=False)
```

```python
import functools

import jax
import jax.numpy as jnp
from jax import lax
from jax.experimental import pallas as pl
from jax.experimental.pallas import tpu as pltpu
from jax.sharding import PartitionSpec as P

EPS = 1e-6
MASKED = -1e30
MESH = pl.DeviceIdType.MESH
F32 = jnp.float32
BF16 = jnp.bfloat16
NT = (((1,), (1,)), ((), ()))
NS = 10


def rms(x, gain):
    mean_sq = jnp.mean(x * x, axis=-1, keepdims=True)
    return (x * lax.rsqrt(mean_sq + EPS) * gain).astype(BF16)


def kernel(caps, hid_hbm, k_hbm, v_hbm, len_hbm, r_hbm, u_hbm, w_hbm, ga_hbm, wq_hbm, wk_hbm, wv_hbm, wo_hbm, gm_hbm, wu_hbm, wd_hbm,
           out_ref, flag_ref,
           hid_ref, len_ref, u_ref, w_ref, ga_ref, gm_ref, ring, rel_own, rel_par, content, probs, p_extra, wo, wu, wd, qc_bd, k_new, v_new, rows_acc, part, asend, arecv, dsend, drecv,
           ring_sem, wt_sem, r_sem, par_sem, cro_send, cro_recv, dia_send, dia_recv, part_send, part_recv, ex_sem, table, *far_refs):
    nb, nh, width = content.shape
    feat = k_hbm.shape[1]
    hd = feat // nh
    even, odd = caps
    stages = len(even) - 1
    group = nb // stages
    compact = even[-1] < nb
    rel_cro, rel_dia = far_refs[:stages], far_refs[stages:2 * stages]
    rel_send = far_refs[-1] if compact else rel_own
    sp = lax.axis_index("sp")
    tp = lax.axis_index("tp")
    chip = sp // 2
    core = lax.rem(sp, 2)
    partner = chip * 2 + (1 - core)
    cross = (1 - chip) * 2 + core
    diag = (1 - chip) * 2 + (1 - core)

    def by_core(c, a, b):
        return a + (b - a) * c

    def size(g, c):
        return by_core(c, even[g + 1] - even[g], odd[g + 1] - odd[g])

    def begin(g, c):
        return by_core(c, even[g], odd[g])

    barrier = pltpu.get_barrier_semaphore()
    for peer in (partner, cross, diag):
        pl.semaphore_signal(barrier, inc=1, device_id={"sp": peer}, device_id_type=MESH)
    pl.semaphore_signal(barrier, inc=1, device_id={"tp": 1 - tp}, device_id_type=MESH)

    def load(src, dst, sem):
        return pltpu.make_async_copy(src, dst, sem)

    def k_load(b):
        return load(k_hbm.at[b], ring.at[lax.rem(b, NS)], ring_sem.at[lax.rem(b, NS)])

    def v_load(b):
        slot = lax.rem(b + nb, NS)
        return load(v_hbm.at[b], ring.at[slot], ring_sem.at[slot])

    small = [load(a, b, wt_sem.at[6 + i]) for i, (a, b) in enumerate(((hid_hbm, hid_ref), (ga_hbm, ga_ref), (len_hbm, len_ref), (u_hbm, u_ref), (w_hbm, w_ref), (gm_hbm, gm_ref)))]
    for copy in small:
        copy.start()
    wdt = wq_hbm.shape[1]
    stage = ring.at[NS - 2]
    step = 1024
    r_copies = [load(r_hbm.at[:, pl.ds(c, step)], ring.at[NS - 1, :, pl.ds(c, step)], r_sem.at[c // step]) for c in range(0, width, step)]
    wq_copy = load(wq_hbm, stage.at[:, pl.ds(0, wdt)], wt_sem.at[0])
    wk_copy = load(wk_hbm, stage.at[:, pl.ds(wdt, wdt)], wt_sem.at[1])
    wv_copy = load(wv_hbm, stage.at[:, pl.ds(2 * wdt, wdt)], wt_sem.at[2])
    wo_copy = load(wo_hbm, wo, wt_sem.at[3])
    wu_copy = load(wu_hbm, wu, wt_sem.at[4])
    wd_copy = load(wd_hbm, wd, wt_sem.at[5])
    wq_copy.start()
    for copy in r_copies:
        copy.start()
    wk_copy.start()
    wv_copy.start()
    for b in range(NS - 2):
        k_load(b).start()

    for copy in small:
        copy.wait()
    fits = jnp.int32(1)
    if compact:
        for level, cap in enumerate(caps):
            rank = jnp.int32(0)
            for b in range(nb):
                table[level, b] = rank
                rank = rank + (len_ref[b] >= (2 + level) * width).astype(jnp.int32)
                if (b + 1) % group == 0:
                    fits = jnp.where(rank <= cap[(b + 1) // group], fits, 0)
        reach = [len_ref[b] >= (2 + core) * width for b in range(nb)]
        ranks = [table[core, b] for b in range(nb)]
        chosen = {}
        for g in range(stages):
            for c in range(even[g + 1] - even[g]):
                want = begin(g, core) + c
                chosen[g, c] = functools.reduce(jnp.add, [jnp.where(reach[b] & (ranks[b] == want), b, 0) for b in range(nb)])

    flag_ref[0] = fits
    hidden = hid_ref[...].astype(F32)
    normed = rms(hidden, ga_ref[...][None].astype(F32))

    head_of_row = lax.broadcasted_iota(jnp.int32, (nh, feat), 0)
    head_of_col = lax.broadcasted_iota(jnp.int32, (nh, feat), 1) // hd
    diag_mask = head_of_row == head_of_col
    spread_row = lax.broadcasted_iota(jnp.int32, (hd, feat), 0)
    spread_col = lax.rem(lax.broadcasted_iota(jnp.int32, (hd, feat), 1), hd)
    spread = (spread_row == spread_col).astype(BF16)
    u_wide = jnp.dot(u_ref[...], spread, preferred_element_type=F32)
    w_wide = jnp.dot(w_ref[...], spread, preferred_element_type=F32)

    wq_copy.wait()
    query = lax.dot_general(normed, stage[:, pl.ds(0, wdt)], NT, preferred_element_type=F32).astype(BF16).astype(F32)
    zero_rows = jnp.zeros((nh, feat), F32)
    pos_rows = []
    for b in range(nb):
        row = query[b:b + 1, :]
        qc = jnp.where(diag_mask, row + u_wide, 0.0)
        qc_bd[b] = jnp.concatenate([qc, zero_rows], axis=0).astype(BF16)
        pos_rows.append(jnp.where(diag_mask, row + w_wide, 0.0))
    q_pos = jnp.concatenate(pos_rows, axis=0).astype(BF16)

    for c in range(width // step):
        cols = pl.ds(c * step, step)
        r_copies[c].wait()
        prod = jnp.dot(q_pos, ring[NS - 1, :, cols], preferred_element_type=F32)
        rel_own[:, :, cols] = prod.reshape(nb, nh, step)
    pl.semaphore_wait(barrier, 4)

    par_copy = pltpu.make_async_remote_copy(src_ref=rel_own, dst_ref=rel_par, send_sem=par_sem.at[0], recv_sem=par_sem.at[1],
                                            device_id={"sp": partner}, device_id_type=MESH)

    def cross_copy(g, c):
        i = even[g] + c
        return pltpu.make_async_remote_copy(src_ref=rel_send.at[i], dst_ref=rel_cro[g].at[c], send_sem=cro_send.at[i], recv_sem=cro_recv.at[i],
                                            device_id={"sp": cross}, device_id_type=MESH)

    def forward_copy(g, c):
        i = even[g] + c
        return pltpu.make_async_remote_copy(src_ref=rel_cro[g].at[c], dst_ref=rel_dia[g].at[c], send_sem=dia_send.at[i], recv_sem=dia_recv.at[i],
                                            device_id={"sp": partner}, device_id_type=MESH)

    for g in range(stages):
        for c in range(even[g + 1] - even[g]):
            if compact:
                rel_send[even[g] + c] = rel_own[chosen[g, c]]

            @pl.when(c < size(g, core))
            def _():
                cross_copy(g, c).start()
        if g == 0:
            par_copy.start()

    wk_copy.wait()
    k_new[...] = lax.dot_general(normed, stage[:, pl.ds(wdt, wdt)], NT, preferred_element_type=F32).astype(BF16).astype(F32)
    wv_copy.wait()
    v_new[...] = lax.dot_general(normed, stage[:, pl.ds(2 * wdt, wdt)], NT, preferred_element_type=F32).astype(BF16).astype(F32)
    for b in range(NS - 2, NS):
        k_load(b).start()

    def arrive(g, c):
        @pl.when((c >= 0) & (c < size(g, core)))
        def _():
            cross_copy(g, c).wait()
            forward_copy(g, c).start()

    @pl.loop(0, nb)
    def _(b):
        @pl.when(b == nb - 3)
        def _():
            for c in range(rel_cro[0].shape[0]):
                arrive(0, c)

        k_load(b).wait()
        content[b] = jnp.dot(qc_bd[b], ring[lax.rem(b, NS)], preferred_element_type=F32)[:nh]

        @pl.when(b < nb - NS)
        def _():
            k_load(b + NS).start()

        @pl.when(b >= nb - NS)
        def _():
            v_load(b + NS - nb).start()

    par_copy.wait()

    lane = lax.broadcasted_iota(jnp.int32, (nh, width), 1)
    back = 127 - lax.broadcasted_iota(jnp.int32, (nh, 128), 1)
    stat_lane = lax.broadcasted_iota(jnp.int32, (nh, 128), 1)
    stat_row = lax.broadcasted_iota(jnp.int32, (nh, 128), 0)

    def pick(rows, g, b, level):
        if not compact:
            return rows[g][b - g * group]
        unit = table[level, b]
        x = rows[0][jnp.minimum(unit, rows[0].shape[0] - 1)]
        for h in range(1, g + 1):
            local = unit - begin(h, level)
            x = jnp.where(local >= 0, rows[h][jnp.clip(local, 0, rows[h].shape[0] - 1)], x)
        return x

    def score(g, b, slot):
        length = len_ref[b]
        high = length // width
        low = length - high * width
        first = high - sp
        upper = lane <= low
        far = pick(rel_cro, g, b, core)
        farther = pick(rel_dia, g, b, 1 - core)
        comb = jnp.zeros((nh, width), F32)
        for block, rows in ((sp, rel_own[b]), (partner, rel_par[b]), (cross, far), (diag, farther)):
            want = jnp.where(upper, first, first - 1) == block
            comb = jnp.where(want, rows, comb)
        pieces = [jnp.take_along_axis(comb[:, 128 * c:128 * c + 128], back, axis=1) for c in range(width // 128)]
        relative = pltpu.roll(jnp.concatenate(pieces[::-1], axis=1), lax.rem(low + 1, width), axis=1)
        here = length - sp * width
        valid = lane <= here
        is_new = lane == here
        q_rows = qc_bd[b][:nh].astype(F32)
        s_new = jnp.sum(q_rows * k_new[pl.ds(b, 1), :], axis=1, keepdims=True)
        scores = jnp.where(is_new, s_new, content[b]) + relative
        scores = jnp.where(valid, scores * (hd ** -0.5), MASKED)
        top = jnp.max(scores, axis=1, keepdims=True)
        weights = jnp.where(valid, jnp.exp(scores - top), 0.0)
        total = jnp.sum(weights, axis=1, keepdims=True)
        p_new = jnp.sum(jnp.where(is_new, weights, 0.0), axis=1, keepdims=True).astype(BF16).astype(F32)
        probs[slot] = jnp.where(is_new, 0.0, weights).astype(BF16)
        p_extra[slot] = jnp.broadcast_to(p_new, (nh, 128))
        stats = jnp.where(stat_lane == stat_row, top, jnp.where(stat_lane == stat_row + nh, total, 0.0))
        rows_acc[b, :, pl.ds(feat, 128)] = jnp.sum(stats, axis=0, keepdims=True)

    def mix(b, slot):
        mixed = lax.dot_general(probs[slot], ring[lax.rem(b + nb, NS)], NT, preferred_element_type=F32)
        mixed = mixed + p_extra[slot][:, :1] * v_new[pl.ds(b, 1), :]
        rows_acc[b, :, pl.ds(0, feat)] = jnp.sum(jnp.where(diag_mask, mixed, 0.0), axis=0, keepdims=True)

    def settle(g):
        for c in range(rel_cro[g].shape[0]):
            @pl.when(c < size(g, core))
            def _():
                forward_copy(g, c).wait_send()

            @pl.when(c < size(g, 1 - core))
            def _():
                forward_copy(g, c).wait_recv()

    settle(0)
    score(0, 0, 0)

    for g in range(stages):
        late = rel_cro[g + 1].shape[0] if g + 1 < stages else 0
        first_step = max(g * group - 1, 0)
        last_step = g * group + group - 2
        if g > 0:
            settle(g)
        for c in range(late - (last_step - first_step + 1)):
            arrive(g + 1, c)

        @pl.loop(first_step, last_step + 1)
        def _(i):
            if late:
                arrive(g + 1, i - last_step + late - 1)

            v_load(i).wait()
            mix(i, lax.rem(i, 2))
            score(g, i + 1, lax.rem(i + 1, 2))

            @pl.when(i < nb - NS)
            def _():
                v_load(i + NS).start()

    wo_copy.start()
    wu_copy.start()
    wd_copy.start()
    v_load(nb - 1).wait()
    mix(nb - 1, (nb - 1) % 2)

    for b in range(nb):
        part[0, b:b + 1, :] = rows_acc[b]
    part_copies = []
    for j, peer in ((1, partner), (2, cross), (3, diag)):
        part_copies.append(pltpu.make_async_remote_copy(src_ref=part.at[0], dst_ref=part.at[j], send_sem=part_send.at[j], recv_sem=part_recv.at[j],
                                                        device_id={"sp": peer}, device_id_type=MESH))
    for copy in part_copies:
        copy.start()
    for copy in part_copies:
        copy.wait()

    blocks = []
    for s in range(4):
        j = lax.rem(chip + s // 2, 2) * 2 + lax.rem(core + s % 2, 2)
        blocks.append(part[j])
    tops = [x[:, feat:] for x in blocks]
    top_all = functools.reduce(jnp.maximum, tops)
    scale = [jnp.exp(t - top_all) for t in tops]
    total = sum(s * pltpu.roll(t, 128 - nh, axis=1) for s, t in zip(scale, tops))
    lane_head = lax.broadcasted_iota(jnp.int32, (nb, 128), 1) // hd
    context = jnp.zeros((nb, feat), F32)
    for s, x in zip(scale, blocks):
        factor = s / total
        wide = jnp.concatenate([jnp.take_along_axis(factor, lane_head + c * (128 // hd), axis=1) for c in range(feat // 128)], axis=1)
        context = context + wide * x[:, :feat]

    def exchange(send, recv, j):
        return pltpu.make_async_remote_copy(src_ref=send, dst_ref=recv, send_sem=ex_sem.at[2 * j], recv_sem=ex_sem.at[2 * j + 1],
                                            device_id={"tp": 1 - tp}, device_id_type=MESH)

    wo_copy.wait()
    attn = jnp.dot(context.astype(BF16), wo[...], preferred_element_type=F32)
    asend[...] = attn
    swap = exchange(asend, arecv, 0)
    swap.start()
    swap.wait()
    middle = (hidden + (attn + arecv[...])).astype(BF16).astype(F32)
    normed_mlp = rms(middle, gm_ref[...][None].astype(F32))
    wu_copy.wait()
    up = jnp.dot(normed_mlp, wu[...], preferred_element_type=F32)
    act = jax.nn.gelu(up, approximate=True).astype(BF16)
    wd_copy.wait()
    down = jnp.dot(act, wd[...], preferred_element_type=F32)
    dsend[...] = down
    swap = exchange(dsend, drecv, 1)
    swap.start()
    swap.wait()
    out_ref[...] = (middle + (down + drecv[...])).astype(BF16)


def solution(mesh):
    spec_cache = P('dp', 'sp', 'tp', None)
    in_specs = (P('dp', None), spec_cache, spec_cache, P('dp'), P('sp', 'tp', None), P('tp', None), P('tp', None), P(None), P(None, 'tp', None), P(None, 'tp', None), P(None, 'tp', None), P('tp', None, None), P(None), P(None, 'tp'), P('tp', None))

    def layer_step(hidden, k_cache, v_cache, lengths, rel_table, u_bias, w_bias, g_attn, w_query, w_key, w_value, w_out, g_mlp, w_up, w_down):
        nb, width, nh, hd = k_cache.shape
        feat = nh * hd
        model = hidden.shape[1]
        k_t = k_cache.transpose(0, 2, 3, 1).reshape(nb, feat, width)
        v_t = v_cache.transpose(0, 2, 3, 1).reshape(nb, feat, width)
        r_t = rel_table.transpose(1, 2, 0).reshape(feat, width)
        proj = [w.transpose(1, 2, 0).reshape(feat, model) for w in (w_query, w_key, w_value)]
        vmem = pl.BlockSpec(memory_space=pltpu.VMEM)
        hbm = pl.BlockSpec(memory_space=pl.ANY)
        dma = pltpu.SemaphoreType.DMA
        full = 2 * ((0, nb),)
        tight = (0, 4, 7, 10, 13), (0, 3, 5, 7, 8)

        def call(caps, *operands):
            compact = caps != full
            rows = caps[0][-1]
            return pl.pallas_call(
                functools.partial(kernel, caps),
                out_shape=(jax.ShapeDtypeStruct((nb, model), BF16), jax.ShapeDtypeStruct((1,), jnp.int32)),
                in_specs=15 * [hbm],
                out_specs=(vmem, pl.BlockSpec(memory_space=pltpu.SMEM)),
                scratch_shapes=[
                    pltpu.VMEM(hidden.shape, BF16),
                    pltpu.SMEM(lengths.shape, jnp.int32),
                    pltpu.VMEM(u_bias.shape, BF16),
                    pltpu.VMEM(w_bias.shape, BF16),
                    pltpu.VMEM(g_attn.shape, BF16),
                    pltpu.VMEM(g_mlp.shape, BF16),
                    pltpu.VMEM((NS, feat, width), BF16),
                    pltpu.VMEM((nb, nh, width), F32),
                    pltpu.VMEM((nb, nh, width), F32),
                    pltpu.VMEM((nb, nh, width), F32),
                    pltpu.VMEM((2, nh, width), BF16),
                    pltpu.VMEM((2, nh, 128), F32),
                    pltpu.VMEM((feat, model), BF16),
                    pltpu.VMEM(w_up.shape, BF16),
                    pltpu.VMEM(w_down.shape, BF16),
                    pltpu.VMEM((nb, 16, feat), BF16),
                    pltpu.VMEM((nb, feat), F32),
                    pltpu.VMEM((nb, feat), F32),
                    pltpu.VMEM((nb, 1, feat + 128), F32),
                    pltpu.VMEM((4, nb, feat + 128), F32),
                    pltpu.VMEM((nb, model), F32),
                    pltpu.VMEM((nb, model), F32),
                    pltpu.VMEM((nb, model), F32),
                    pltpu.VMEM((nb, model), F32),
                    dma((NS,)), dma((12,)), dma((4,)), dma((2,)), dma((rows,)), dma((rows,)), dma((rows,)), dma((rows,)), dma((4,)), dma((4,)), dma((4,)),
                    pltpu.SMEM((2, nb), jnp.int32),
                ] + 2 * [pltpu.VMEM((b - a, nh, width), F32) for a, b in zip(caps[0], caps[0][1:])] + ([pltpu.VMEM((rows, nh, width), F32)] if compact else []),
                compiler_params=pltpu.CompilerParams(collective_id=int(compact), has_side_effects=True, vmem_limit_bytes=67043328),
            )(*operands)

        operands = (hidden, k_t, v_t, lengths, r_t, u_bias, w_bias, g_attn, *proj, w_out.reshape(feat, model), g_mlp, w_up, w_down)
        out, fits = call(tight, *operands)
        return lax.cond(fits[0] > 0, lambda *_: out, lambda *full_operands: call(full, *full_operands)[0], *operands)

    return jax.shard_map(layer_step, mesh=mesh, in_specs=in_specs, out_specs=P('dp', None), check_vma=False)
```

```python
import functools

import jax
import jax.numpy as jnp
from jax import lax
from jax.experimental import pallas as pl
from jax.experimental.pallas import tpu as pltpu
from jax.sharding import PartitionSpec as P

EPS = 1e-6
MASKED = -1e30
MESH = pl.DeviceIdType.MESH
F32 = jnp.float32
BF16 = jnp.bfloat16
NT = (((1,), (1,)), ((), ()))
NS = 10
LATE = 4


def rms(x, gain):
    mean_sq = jnp.mean(x * x, axis=-1, keepdims=True)
    return (x * lax.rsqrt(mean_sq + EPS) * gain).astype(BF16)


def kernel(caps, hid_hbm, k_hbm, v_hbm, len_hbm, r_hbm, u_hbm, w_hbm, ga_hbm, wq_hbm, wk_hbm, wv_hbm, wo_hbm, gm_hbm, wu_hbm, wd_hbm,
           out_ref, flag_ref,
           hid_ref, len_ref, u_ref, w_ref, ga_ref, gm_ref, ring, rel_own, rel_par, content, probs, p_extra, wo, wu, wd, qc_bd, k_new, v_new, rows_acc, part_e, part_l, asend_e, arecv_e, asend_l, arecv_l, dsend_e, drecv_e, dsend_l, drecv_l,
           ring_sem, wt_sem, r_sem, par_sem, cro_send, cro_recv, dia_send, dia_recv, part_send, part_recv, att_sem, ex_send, ex_recv, table, *far_refs):
    nb, nh, width = content.shape
    feat = k_hbm.shape[1]
    hd = feat // nh
    even, odd = caps
    stages = len(even) - 1
    group = nb // stages
    compact = even[-1] < nb
    rel_cro, rel_dia = far_refs[:stages], far_refs[stages:2 * stages]
    rel_send = far_refs[-1] if compact else rel_own
    sp = lax.axis_index("sp")
    tp = lax.axis_index("tp")
    chip = sp // 2
    core = lax.rem(sp, 2)
    partner = chip * 2 + (1 - core)
    cross = (1 - chip) * 2 + core
    diag = (1 - chip) * 2 + (1 - core)

    def by_core(c, a, b):
        return a + (b - a) * c

    def size(g, c):
        return by_core(c, even[g + 1] - even[g], odd[g + 1] - odd[g])

    def begin(g, c):
        return by_core(c, even[g], odd[g])

    barrier = pltpu.get_barrier_semaphore()
    for peer in (partner, cross, diag):
        pl.semaphore_signal(barrier, inc=1, device_id={"sp": peer}, device_id_type=MESH)
    pl.semaphore_signal(barrier, inc=1, device_id={"tp": 1 - tp}, device_id_type=MESH)

    def load(src, dst, sem):
        return pltpu.make_async_copy(src, dst, sem)

    def k_load(b):
        return load(k_hbm.at[b], ring.at[lax.rem(b, NS)], ring_sem.at[lax.rem(b, NS)])

    def v_load(b):
        slot = lax.rem(b + nb, NS)
        return load(v_hbm.at[b], ring.at[slot], ring_sem.at[slot])

    small = [load(a, b, wt_sem.at[6 + i]) for i, (a, b) in enumerate(((hid_hbm, hid_ref), (ga_hbm, ga_ref), (len_hbm, len_ref), (u_hbm, u_ref), (w_hbm, w_ref), (gm_hbm, gm_ref)))]
    for copy in small:
        copy.start()
    wdt = wq_hbm.shape[1]
    stage = ring.at[NS - 2]
    step = 1024
    r_copies = [load(r_hbm.at[:, pl.ds(c, step)], ring.at[NS - 1, :, pl.ds(c, step)], r_sem.at[c // step]) for c in range(0, width, step)]
    wq_copy = load(wq_hbm, stage.at[:, pl.ds(0, wdt)], wt_sem.at[0])
    wk_copy = load(wk_hbm, stage.at[:, pl.ds(wdt, wdt)], wt_sem.at[1])
    wv_copy = load(wv_hbm, stage.at[:, pl.ds(2 * wdt, wdt)], wt_sem.at[2])
    wo_copy = load(wo_hbm, wo, wt_sem.at[3])
    wu_copy = load(wu_hbm, wu, wt_sem.at[4])
    wd_copy = load(wd_hbm, wd, wt_sem.at[5])
    wq_copy.start()
    for copy in r_copies:
        copy.start()
    wk_copy.start()
    wv_copy.start()
    for b in range(NS - 2):
        k_load(b).start()

    for copy in small:
        copy.wait()
    fits = jnp.int32(1)
    if compact:
        for level, cap in enumerate(caps):
            rank = jnp.int32(0)
            for b in range(nb):
                table[level, b] = rank
                rank = rank + (len_ref[b] >= (2 + level) * width).astype(jnp.int32)
                if (b + 1) % group == 0:
                    fits = jnp.where(rank <= cap[(b + 1) // group], fits, 0)
        reach = [len_ref[b] >= (2 + core) * width for b in range(nb)]
        ranks = [table[core, b] for b in range(nb)]
        chosen = {}
        for g in range(stages):
            for c in range(even[g + 1] - even[g]):
                want = begin(g, core) + c
                chosen[g, c] = functools.reduce(jnp.add, [jnp.where(reach[b] & (ranks[b] == want), b, 0) for b in range(nb)])

    flag_ref[0] = fits
    hidden = hid_ref[...].astype(F32)
    normed = rms(hidden, ga_ref[...][None].astype(F32))

    head_of_row = lax.broadcasted_iota(jnp.int32, (nh, feat), 0)
    head_of_col = lax.broadcasted_iota(jnp.int32, (nh, feat), 1) // hd
    diag_mask = head_of_row == head_of_col
    spread_row = lax.broadcasted_iota(jnp.int32, (hd, feat), 0)
    spread_col = lax.rem(lax.broadcasted_iota(jnp.int32, (hd, feat), 1), hd)
    spread = (spread_row == spread_col).astype(BF16)
    u_wide = jnp.dot(u_ref[...], spread, preferred_element_type=F32)
    w_wide = jnp.dot(w_ref[...], spread, preferred_element_type=F32)

    wq_copy.wait()
    query = lax.dot_general(normed, stage[:, pl.ds(0, wdt)], NT, preferred_element_type=F32).astype(BF16).astype(F32)
    zero_rows = jnp.zeros((nh, feat), F32)
    pos_rows = []
    for b in range(nb):
        row = query[b:b + 1, :]
        qc = jnp.where(diag_mask, row + u_wide, 0.0)
        qc_bd[b] = jnp.concatenate([qc, zero_rows], axis=0).astype(BF16)
        pos_rows.append(jnp.where(diag_mask, row + w_wide, 0.0))
    q_pos = jnp.concatenate(pos_rows, axis=0).astype(BF16)

    for c in range(width // step):
        cols = pl.ds(c * step, step)
        r_copies[c].wait()
        prod = jnp.dot(q_pos, ring[NS - 1, :, cols], preferred_element_type=F32)
        rel_own[:, :, cols] = prod.reshape(nb, nh, step)
    pl.semaphore_wait(barrier, 4)

    par_copy = pltpu.make_async_remote_copy(src_ref=rel_own, dst_ref=rel_par, send_sem=par_sem.at[0], recv_sem=par_sem.at[1],
                                            device_id={"sp": partner}, device_id_type=MESH)

    def cross_copy(g, c):
        i = even[g] + c
        return pltpu.make_async_remote_copy(src_ref=rel_send.at[i], dst_ref=rel_cro[g].at[c], send_sem=cro_send.at[i], recv_sem=cro_recv.at[i],
                                            device_id={"sp": cross}, device_id_type=MESH)

    def forward_copy(g, c):
        i = even[g] + c
        return pltpu.make_async_remote_copy(src_ref=rel_cro[g].at[c], dst_ref=rel_dia[g].at[c], send_sem=dia_send.at[i], recv_sem=dia_recv.at[i],
                                            device_id={"sp": partner}, device_id_type=MESH)

    for g in range(stages):
        for c in range(even[g + 1] - even[g]):
            if compact:
                rel_send[even[g] + c] = rel_own[chosen[g, c]]

            @pl.when(c < size(g, core))
            def _():
                cross_copy(g, c).start()
        if g == 0:
            par_copy.start()

    wk_copy.wait()
    k_new[...] = lax.dot_general(normed, stage[:, pl.ds(wdt, wdt)], NT, preferred_element_type=F32).astype(BF16).astype(F32)
    wv_copy.wait()
    v_new[...] = lax.dot_general(normed, stage[:, pl.ds(2 * wdt, wdt)], NT, preferred_element_type=F32).astype(BF16).astype(F32)
    for b in range(NS - 2, NS):
        k_load(b).start()

    def arrive(g, c):
        @pl.when((c >= 0) & (c < size(g, core)))
        def _():
            cross_copy(g, c).wait()
            forward_copy(g, c).start()

    @pl.loop(0, nb)
    def _(b):
        @pl.when(b == nb - 3)
        def _():
            for c in range(rel_cro[0].shape[0]):
                arrive(0, c)

        k_load(b).wait()
        content[b] = jnp.dot(qc_bd[b], ring[lax.rem(b, NS)], preferred_element_type=F32)[:nh]

        @pl.when(b < nb - NS)
        def _():
            k_load(b + NS).start()

        @pl.when(b >= nb - NS)
        def _():
            v_load(b + NS - nb).start()

    wo_copy.start()
    par_copy.wait()

    lane = lax.broadcasted_iota(jnp.int32, (nh, width), 1)
    back = 127 - lax.broadcasted_iota(jnp.int32, (nh, 128), 1)
    stat_lane = lax.broadcasted_iota(jnp.int32, (nh, 128), 1)
    stat_row = lax.broadcasted_iota(jnp.int32, (nh, 128), 0)

    def pick(rows, g, b, level):
        if not compact:
            return rows[g][b - g * group]
        unit = table[level, b]
        x = rows[0][jnp.minimum(unit, rows[0].shape[0] - 1)]
        for h in range(1, g + 1):
            local = unit - begin(h, level)
            x = jnp.where(local >= 0, rows[h][jnp.clip(local, 0, rows[h].shape[0] - 1)], x)
        return x

    def score(g, b, slot):
        length = len_ref[b]
        high = length // width
        low = length - high * width
        first = high - sp
        upper = lane <= low
        far = pick(rel_cro, g, b, core)
        farther = pick(rel_dia, g, b, 1 - core)
        comb = jnp.zeros((nh, width), F32)
        for block, rows in ((sp, rel_own[b]), (partner, rel_par[b]), (cross, far), (diag, farther)):
            want = jnp.where(upper, first, first - 1) == block
            comb = jnp.where(want, rows, comb)
        pieces = [jnp.take_along_axis(comb[:, 128 * c:128 * c + 128], back, axis=1) for c in range(width // 128)]
        relative = pltpu.roll(jnp.concatenate(pieces[::-1], axis=1), lax.rem(low + 1, width), axis=1)
        here = length - sp * width
        valid = lane <= here
        is_new = lane == here
        q_rows = qc_bd[b][:nh].astype(F32)
        s_new = jnp.sum(q_rows * k_new[pl.ds(b, 1), :], axis=1, keepdims=True)
        scores = jnp.where(is_new, s_new, content[b]) + relative
        scores = jnp.where(valid, scores * (hd ** -0.5), MASKED)
        top = jnp.max(scores, axis=1, keepdims=True)
        weights = jnp.where(valid, jnp.exp(scores - top), 0.0)
        total = jnp.sum(weights, axis=1, keepdims=True)
        p_new = jnp.sum(jnp.where(is_new, weights, 0.0), axis=1, keepdims=True).astype(BF16).astype(F32)
        probs[slot] = jnp.where(is_new, 0.0, weights).astype(BF16)
        p_extra[slot] = jnp.broadcast_to(p_new, (nh, 128))
        stats = jnp.where(stat_lane == stat_row, top, jnp.where(stat_lane == stat_row + nh, total, 0.0))
        rows_acc[b, :, pl.ds(feat, 128)] = jnp.sum(stats, axis=0, keepdims=True)

    def mix(b, slot):
        mixed = lax.dot_general(probs[slot], ring[lax.rem(b + nb, NS)], NT, preferred_element_type=F32)
        mixed = mixed + p_extra[slot][:, :1] * v_new[pl.ds(b, 1), :]
        rows_acc[b, :, pl.ds(0, feat)] = jnp.sum(jnp.where(diag_mask, mixed, 0.0), axis=0, keepdims=True)

    def settle(g):
        for c in range(rel_cro[g].shape[0]):
            @pl.when(c < size(g, core))
            def _():
                forward_copy(g, c).wait_send()

            @pl.when(c < size(g, 1 - core))
            def _():
                forward_copy(g, c).wait_recv()

    settle(0)
    score(0, 0, 0)

    lane_heads = [lax.broadcasted_iota(jnp.int32, (8, 128), 1) // hd + c * (128 // hd) for c in range(feat // 128)]

    def peers(part, k):
        return [pltpu.make_async_remote_copy(src_ref=part.at[0], dst_ref=part.at[j], send_sem=part_send.at[k, j], recv_sem=part_recv.at[k, j],
                                             device_id={"sp": peer}, device_id_type=MESH) for j, peer in ((1, partner), (2, cross), (3, diag))]

    def share(part, k, base):
        for b in range(part.shape[1]):
            part[0, b:b + 1, :] = rows_acc[base + b]
        for copy in peers(part, k):
            copy.start()

    def exchange(send, recv, k):
        return pltpu.make_async_remote_copy(src_ref=send, dst_ref=recv, send_sem=att_sem.at[k, 0], recv_sem=att_sem.at[k, 1],
                                            device_id={"tp": 1 - tp}, device_id_type=MESH)

    def merge(part, k):
        for copy in peers(part, k):
            copy.wait()
        blocks = []
        for s in range(4):
            j = lax.rem(chip + s // 2, 2) * 2 + lax.rem(core + s % 2, 2)
            blocks.append(part[j])
        tops = [x[:, feat:] for x in blocks]
        top_all = functools.reduce(jnp.maximum, tops)
        scale = [jnp.exp(t - top_all) for t in tops]
        total = sum(s * pltpu.roll(t, 128 - nh, axis=1) for s, t in zip(scale, tops))
        context = jnp.zeros((part.shape[1], feat), F32)
        for s, x in zip(scale, blocks):
            factor = s / total
            wide = jnp.concatenate([sum(jnp.where(lane_heads[c][:1] == h, factor[:, h:h + 1], 0.0) for h in range(c * (128 // hd), (c + 1) * (128 // hd))) for c in range(feat // 128)], axis=1)
            context = context + wide * x[:, :feat]
        return jnp.dot(context.astype(BF16), wo[...], preferred_element_type=F32)

    def finish_early():
        wo_copy.wait()
        asend_e[...] = merge(part_e, 0)
        exchange(asend_e, arecv_e, 0).start()

    for g in range(stages):
        late = rel_cro[g + 1].shape[0] if g + 1 < stages else 0
        first_step = max(g * group - 1, 0)
        last_step = g * group + group - 2
        if g > 0:
            settle(g)
        for c in range(late - (last_step - first_step + 1)):
            arrive(g + 1, c)

        @pl.loop(first_step, last_step + 1)
        def _(i):
            if late:
                arrive(g + 1, i - last_step + late - 1)

            if g == stages - 1:
                @pl.when(i == nb - LATE)
                def _():
                    share(part_e, 0, 0)

            v_load(i).wait()
            mix(i, lax.rem(i, 2))
            score(g, i + 1, lax.rem(i + 1, 2))

            @pl.when(i < nb - NS)
            def _():
                v_load(i + NS).start()

    wu_copy.start()
    wd_copy.start()
    v_load(nb - 1).wait()
    mix(nb - 1, (nb - 1) % 2)

    def down_copies(send, recv, k):
        return [pltpu.make_async_remote_copy(src_ref=send.at[c], dst_ref=recv.at[c], send_sem=ex_send.at[k, c], recv_sem=ex_recv.at[k, c],
                                             device_id={"tp": 1 - tp}, device_id_type=MESH) for c in range(send.shape[0])]

    def mlp(rows, attn, send, recv, k):
        middle = (rows + attn).astype(BF16).astype(F32)
        normed_mlp = rms(middle, gm_ref[...][None].astype(F32))
        up = jnp.dot(normed_mlp, wu[...], preferred_element_type=F32)
        act = jax.nn.gelu(up, approximate=True).astype(BF16)
        cols = send.shape[2]
        for c, copy in enumerate(down_copies(send, recv, k)):
            send[c] = jnp.dot(act, wd[:, c * cols:(c + 1) * cols], preferred_element_type=F32)
            copy.start()
        return middle

    def finish(middle, send, recv, k):
        done = []
        cols = send.shape[2]
        for c, copy in enumerate(down_copies(send, recv, k)):
            copy.wait()
            done.append(middle[:, c * cols:(c + 1) * cols] + (send[c] + recv[c]))
        return jnp.concatenate(done, axis=1)

    cut = nb - LATE
    share(part_l, 1, cut)
    finish_early()
    asend_l[...] = merge(part_l, 1)
    exchange(asend_l, arecv_l, 1).start()
    exchange(asend_e, arecv_e, 0).wait()
    wu_copy.wait()
    wd_copy.wait()
    middle_e = mlp(hidden[:cut], asend_e[...] + arecv_e[...], dsend_e, drecv_e, 0)
    exchange(asend_l, arecv_l, 1).wait()
    middle_l = mlp(hidden[cut:], asend_l[...] + arecv_l[...], dsend_l, drecv_l, 1)
    first = finish(middle_e, dsend_e, drecv_e, 0)
    last = finish(middle_l, dsend_l, drecv_l, 1)
    out_ref[...] = jnp.concatenate([first, last], axis=0).astype(BF16)


def solution(mesh):
    spec_cache = P('dp', 'sp', 'tp', None)
    in_specs = (P('dp', None), spec_cache, spec_cache, P('dp'), P('sp', 'tp', None), P('tp', None), P('tp', None), P(None), P(None, 'tp', None), P(None, 'tp', None), P(None, 'tp', None), P('tp', None, None), P(None), P(None, 'tp'), P('tp', None))

    def layer_step(hidden, k_cache, v_cache, lengths, rel_table, u_bias, w_bias, g_attn, w_query, w_key, w_value, w_out, g_mlp, w_up, w_down):
        nb, width, nh, hd = k_cache.shape
        feat = nh * hd
        model = hidden.shape[1]
        k_t = k_cache.transpose(0, 2, 3, 1).reshape(nb, feat, width)
        v_t = v_cache.transpose(0, 2, 3, 1).reshape(nb, feat, width)
        r_t = rel_table.transpose(1, 2, 0).reshape(feat, width)
        proj = [w.transpose(1, 2, 0).reshape(feat, model) for w in (w_query, w_key, w_value)]
        vmem = pl.BlockSpec(memory_space=pltpu.VMEM)
        hbm = pl.BlockSpec(memory_space=pl.ANY)
        dma = pltpu.SemaphoreType.DMA
        full = 2 * ((0, nb),)
        tight = (0, 4, 7, 10, 13), (0, 3, 5, 7, 8)

        def call(caps, *operands):
            compact = caps != full
            rows = caps[0][-1]
            return pl.pallas_call(
                functools.partial(kernel, caps),
                out_shape=(jax.ShapeDtypeStruct((nb, model), BF16), jax.ShapeDtypeStruct((1,), jnp.int32)),
                in_specs=15 * [hbm],
                out_specs=(vmem, pl.BlockSpec(memory_space=pltpu.SMEM)),
                scratch_shapes=[
                    pltpu.VMEM(hidden.shape, BF16),
                    pltpu.SMEM(lengths.shape, jnp.int32),
                    pltpu.VMEM(u_bias.shape, BF16),
                    pltpu.VMEM(w_bias.shape, BF16),
                    pltpu.VMEM(g_attn.shape, BF16),
                    pltpu.VMEM(g_mlp.shape, BF16),
                    pltpu.VMEM((NS, feat, width), BF16),
                    pltpu.VMEM((nb, nh, width), F32),
                    pltpu.VMEM((nb, nh, width), F32),
                    pltpu.VMEM((nb, nh, width), F32),
                    pltpu.VMEM((2, nh, width), BF16),
                    pltpu.VMEM((2, nh, 128), F32),
                    pltpu.VMEM((feat, model), BF16),
                    pltpu.VMEM(w_up.shape, BF16),
                    pltpu.VMEM(w_down.shape, BF16),
                    pltpu.VMEM((nb, 16, feat), BF16),
                    pltpu.VMEM((nb, feat), F32),
                    pltpu.VMEM((nb, feat), F32),
                    pltpu.VMEM((nb, 1, feat + 128), F32),
                    pltpu.VMEM((4, nb - LATE, feat + 128), F32),
                    pltpu.VMEM((4, LATE, feat + 128), F32),
                    pltpu.VMEM((nb - LATE, model), F32),
                    pltpu.VMEM((nb - LATE, model), F32),
                    pltpu.VMEM((LATE, model), F32),
                    pltpu.VMEM((LATE, model), F32),
                    pltpu.VMEM((2, nb - LATE, model // 2), F32),
                    pltpu.VMEM((2, nb - LATE, model // 2), F32),
                    pltpu.VMEM((2, LATE, model // 2), F32),
                    pltpu.VMEM((2, LATE, model // 2), F32),
                    dma((NS,)), dma((12,)), dma((4,)), dma((2,)), dma((rows,)), dma((rows,)), dma((rows,)), dma((rows,)), dma((2, 4)), dma((2, 4)), dma((2, 2)), dma((2, 2)), dma((2, 2)),
                    pltpu.SMEM((2, nb), jnp.int32),
                ] + 2 * [pltpu.VMEM((b - a, nh, width), F32) for a, b in zip(caps[0], caps[0][1:])] + ([pltpu.VMEM((rows, nh, width), F32)] if compact else []),
                compiler_params=pltpu.CompilerParams(collective_id=int(compact), has_side_effects=True, vmem_limit_bytes=67043328),
            )(*operands)

        operands = (hidden, k_t, v_t, lengths, r_t, u_bias, w_bias, g_attn, *proj, w_out.reshape(feat, model), g_mlp, w_up, w_down)
        out, fits = call(tight, *operands)
        return lax.cond(fits[0] > 0, lambda *_: out, lambda *full_operands: call(full, *full_operands)[0], *operands)

    return jax.shard_map(layer_step, mesh=mesh, in_specs=in_specs, out_specs=P('dp', None), check_vma=False)
```

```python
import functools

import jax
import jax.numpy as jnp
from jax import lax
from jax.experimental import pallas as pl
from jax.experimental.pallas import tpu as pltpu
from jax.sharding import PartitionSpec as P

EPS = 1e-6
MASKED = -1e30
MESH = pl.DeviceIdType.MESH
F32 = jnp.float32
BF16 = jnp.bfloat16
NT = (((1,), (1,)), ((), ()))
NS = 8
LATE = 4


def rms(x, gain):
    mean_sq = jnp.mean(x * x, axis=-1, keepdims=True)
    return (x * lax.rsqrt(mean_sq + EPS) * gain).astype(BF16)


def kernel(caps, hid_hbm, k_hbm, v_hbm, len_hbm, r_hbm, u_hbm, w_hbm, ga_hbm, wq_hbm, wk_hbm, wv_hbm, wo_hbm, gm_hbm, wu_hbm, wd_hbm,
           out_ref, flag_ref,
           hid_ref, len_ref, u_ref, w_ref, ga_ref, gm_ref, ring, rel_own, rel_par, content, probs, p_extra, wo, wu, wd, qc_bd, k_new, v_new, rows_acc, part_e, part_l, asend_e, arecv_e, asend_l, arecv_l, dsend_e, drecv_e, dsend_l, drecv_l,
           ring_sem, wt_sem, r_sem, par_sem, cro_send, cro_recv, dia_send, dia_recv, part_send, part_recv, att_sem, ex_send, ex_recv, table, *far_refs):
    nb, nh, width = content.shape
    feat = k_hbm.shape[1]
    hd = feat // nh
    even, odd = caps
    stages = len(even) - 1
    group = nb // stages
    compact = even[-1] < nb
    rel_cro, rel_dia = far_refs[:stages], far_refs[stages:2 * stages]
    rel_send = far_refs[-1] if compact else rel_own
    sp = lax.axis_index("sp")
    tp = lax.axis_index("tp")
    chip = sp // 2
    core = lax.rem(sp, 2)
    partner = chip * 2 + (1 - core)
    cross = (1 - chip) * 2 + core
    diag = (1 - chip) * 2 + (1 - core)

    def by_core(c, a, b):
        return a + (b - a) * c

    def size(g, c):
        return by_core(c, even[g + 1] - even[g], odd[g + 1] - odd[g])

    def begin(g, c):
        return by_core(c, even[g], odd[g])

    barrier = pltpu.get_barrier_semaphore()
    for peer in (partner, cross, diag):
        pl.semaphore_signal(barrier, inc=1, device_id={"sp": peer}, device_id_type=MESH)
    pl.semaphore_signal(barrier, inc=1, device_id={"tp": 1 - tp}, device_id_type=MESH)

    def load(src, dst, sem):
        return pltpu.make_async_copy(src, dst, sem)

    def k_load(b):
        return load(k_hbm.at[b], ring.at[lax.rem(b, NS)], ring_sem.at[lax.rem(b, NS)])

    def v_load(b):
        slot = lax.rem(b + nb, NS)
        return load(v_hbm.at[b], ring.at[slot], ring_sem.at[slot])

    if compact:
        pairs = (hid_hbm, hid_ref), (ga_hbm, ga_ref), (len_hbm, len_ref), (u_hbm, u_ref), (w_hbm, w_ref), (gm_hbm, gm_ref)
        small = [load(a, b, wt_sem.at[6 + i]) for i, (a, b) in enumerate(pairs)]
    else:
        small = []
        hid_ref, ga_ref, len_ref, u_ref, w_ref, gm_ref = hid_hbm, ga_hbm, len_hbm, u_hbm, w_hbm, gm_hbm
    for copy in small:
        copy.start()
    wdt = wq_hbm.shape[1]
    stage = ring.at[NS - 2]
    step = 1024
    r_copies = [load(r_hbm.at[:, pl.ds(c, step)], ring.at[NS - 1, :, pl.ds(c, step)], r_sem.at[c // step]) for c in range(0, width, step)]
    wq_copy = load(wq_hbm, stage.at[:, pl.ds(0, wdt)], wt_sem.at[0])
    wk_copy = load(wk_hbm, stage.at[:, pl.ds(wdt, wdt)], wt_sem.at[1])
    wv_copy = load(wv_hbm, stage.at[:, pl.ds(2 * wdt, wdt)], wt_sem.at[2])
    wo_copy = load(wo_hbm, wo, wt_sem.at[3])
    wu_copy = load(wu_hbm, wu, wt_sem.at[4])
    wd_copy = load(wd_hbm, wd, wt_sem.at[5])
    wq_copy.start()
    for copy in r_copies:
        copy.start()
    wk_copy.start()
    wv_copy.start()
    for b in range(NS - 2):
        k_load(b).start()

    for copy in small:
        copy.wait()
    fits = jnp.int32(1)
    if compact:
        for level, cap in enumerate(caps):
            rank = jnp.int32(0)
            for b in range(nb):
                table[level, b] = rank
                rank = rank + (len_ref[b] >= (2 + level) * width).astype(jnp.int32)
                if (b + 1) % group == 0:
                    fits = jnp.where(rank <= cap[(b + 1) // group], fits, 0)
        reach = [len_ref[b] >= (2 + core) * width for b in range(nb)]
        ranks = [table[core, b] for b in range(nb)]
        chosen = {}
        for g in range(stages):
            for c in range(even[g + 1] - even[g]):
                want = begin(g, core) + c
                chosen[g, c] = functools.reduce(jnp.add, [jnp.where(reach[b] & (ranks[b] == want), b, 0) for b in range(nb)])

    flag_ref[0] = fits
    hidden = hid_ref[...].astype(F32)
    normed = rms(hidden, ga_ref[...][None].astype(F32))

    head_of_row = lax.broadcasted_iota(jnp.int32, (nh, feat), 0)
    head_of_col = lax.broadcasted_iota(jnp.int32, (nh, feat), 1) // hd
    diag_mask = head_of_row == head_of_col
    spread_row = lax.broadcasted_iota(jnp.int32, (hd, feat), 0)
    spread_col = lax.rem(lax.broadcasted_iota(jnp.int32, (hd, feat), 1), hd)
    spread = (spread_row == spread_col).astype(BF16)
    u_wide = jnp.dot(u_ref[...], spread, preferred_element_type=F32)
    w_wide = jnp.dot(w_ref[...], spread, preferred_element_type=F32)

    wq_copy.wait()
    query = lax.dot_general(normed, stage[:, pl.ds(0, wdt)], NT, preferred_element_type=F32).astype(BF16).astype(F32)
    zero_rows = jnp.zeros((nh, feat), F32)
    pos_rows = []
    for b in range(nb):
        row = query[b:b + 1, :]
        qc = jnp.where(diag_mask, row + u_wide, 0.0)
        qc_bd[b] = jnp.concatenate([qc, zero_rows], axis=0).astype(BF16)
        pos_rows.append(jnp.where(diag_mask, row + w_wide, 0.0))
    q_pos = jnp.concatenate(pos_rows, axis=0).astype(BF16)

    for c in range(width // step):
        cols = pl.ds(c * step, step)
        r_copies[c].wait()
        prod = jnp.dot(q_pos, ring[NS - 1, :, cols], preferred_element_type=F32)
        rel_own[:, :, cols] = prod.reshape(nb, nh, step)
    pl.semaphore_wait(barrier, 4)

    par_copy = pltpu.make_async_remote_copy(src_ref=rel_own, dst_ref=rel_par, send_sem=par_sem.at[0], recv_sem=par_sem.at[1],
                                            device_id={"sp": partner}, device_id_type=MESH)

    def cross_copy(g, c):
        i = even[g] + c
        return pltpu.make_async_remote_copy(src_ref=rel_send.at[i], dst_ref=rel_cro[g].at[c], send_sem=cro_send.at[i], recv_sem=cro_recv.at[i],
                                            device_id={"sp": cross}, device_id_type=MESH)

    def forward_copy(g, c):
        i = even[g] + c
        return pltpu.make_async_remote_copy(src_ref=rel_cro[g].at[c], dst_ref=rel_dia[g].at[c], send_sem=dia_send.at[i], recv_sem=dia_recv.at[i],
                                            device_id={"sp": partner}, device_id_type=MESH)

    for g in range(stages):
        for c in range(even[g + 1] - even[g]):
            if compact:
                rel_send[even[g] + c] = rel_own[chosen[g, c]]

            @pl.when(c < size(g, core))
            def _():
                cross_copy(g, c).start()
        if g == 0:
            par_copy.start()

    wk_copy.wait()
    k_new[...] = lax.dot_general(normed, stage[:, pl.ds(wdt, wdt)], NT, preferred_element_type=F32).astype(BF16).astype(F32)
    wv_copy.wait()
    v_new[...] = lax.dot_general(normed, stage[:, pl.ds(2 * wdt, wdt)], NT, preferred_element_type=F32).astype(BF16).astype(F32)
    for b in range(NS - 2, NS):
        k_load(b).start()

    def arrive(g, c):
        @pl.when((c >= 0) & (c < size(g, core)))
        def _():
            cross_copy(g, c).wait()
            forward_copy(g, c).start()

    @pl.loop(0, nb)
    def _(b):
        @pl.when(b == nb - 3)
        def _():
            for c in range(rel_cro[0].shape[0]):
                arrive(0, c)

        k_load(b).wait()
        content[b] = jnp.dot(qc_bd[b], ring[lax.rem(b, NS)], preferred_element_type=F32)[:nh]

        @pl.when(b < nb - NS)
        def _():
            k_load(b + NS).start()

        @pl.when(b >= nb - NS)
        def _():
            v_load(b + NS - nb).start()

    wo_copy.start()
    par_copy.wait()

    lane = lax.broadcasted_iota(jnp.int32, (nh, width), 1)
    back = 127 - lax.broadcasted_iota(jnp.int32, (nh, 128), 1)
    stat_lane = lax.broadcasted_iota(jnp.int32, (nh, 128), 1)
    stat_row = lax.broadcasted_iota(jnp.int32, (nh, 128), 0)

    def pick(rows, g, b, level):
        if not compact:
            return rows[g][b - g * group]
        unit = table[level, b]
        x = rows[0][jnp.minimum(unit, rows[0].shape[0] - 1)]
        for h in range(1, g + 1):
            local = unit - begin(h, level)
            x = jnp.where(local >= 0, rows[h][jnp.clip(local, 0, rows[h].shape[0] - 1)], x)
        return x

    def score(g, b, slot):
        length = len_ref[b]
        high = length // width
        low = length - high * width
        first = high - sp
        upper = lane <= low
        far = pick(rel_cro, g, b, core)
        farther = pick(rel_dia, g, b, 1 - core)
        comb = jnp.zeros((nh, width), F32)
        for block, rows in ((sp, rel_own[b]), (partner, rel_par[b]), (cross, far), (diag, farther)):
            want = jnp.where(upper, first, first - 1) == block
            comb = jnp.where(want, rows, comb)
        pieces = [jnp.take_along_axis(comb[:, 128 * c:128 * c + 128], back, axis=1) for c in range(width // 128)]
        relative = pltpu.roll(jnp.concatenate(pieces[::-1], axis=1), lax.rem(low + 1, width), axis=1)
        here = length - sp * width
        valid = lane <= here
        is_new = lane == here
        q_rows = qc_bd[b][:nh].astype(F32)
        s_new = jnp.sum(q_rows * k_new[pl.ds(b, 1), :], axis=1, keepdims=True)
        scores = jnp.where(is_new, s_new, content[b]) + relative
        scores = jnp.where(valid, scores * (hd ** -0.5), MASKED)
        top = jnp.max(scores, axis=1, keepdims=True)
        weights = jnp.where(valid, jnp.exp(scores - top), 0.0)
        total = jnp.sum(weights, axis=1, keepdims=True)
        p_new = jnp.sum(jnp.where(is_new, weights, 0.0), axis=1, keepdims=True).astype(BF16).astype(F32)
        probs[slot] = jnp.where(is_new, 0.0, weights).astype(BF16)
        p_extra[slot] = jnp.broadcast_to(p_new, (nh, 128))
        stats = jnp.where(stat_lane == stat_row, top, jnp.where(stat_lane == stat_row + nh, total, 0.0))
        rows_acc[b, :, pl.ds(feat, 128)] = jnp.sum(stats, axis=0, keepdims=True)

    def mix(b, slot):
        mixed = lax.dot_general(probs[slot], ring[lax.rem(b + nb, NS)], NT, preferred_element_type=F32)
        mixed = mixed + p_extra[slot][:, :1] * v_new[pl.ds(b, 1), :]
        rows_acc[b, :, pl.ds(0, feat)] = jnp.sum(jnp.where(diag_mask, mixed, 0.0), axis=0, keepdims=True)

    def settle(g):
        for c in range(rel_cro[g].shape[0]):
            @pl.when(c < size(g, core))
            def _():
                forward_copy(g, c).wait_send()

            @pl.when(c < size(g, 1 - core))
            def _():
                forward_copy(g, c).wait_recv()

    settle(0)
    score(0, 0, 0)

    lane_heads = [lax.broadcasted_iota(jnp.int32, (8, 128), 1) // hd + c * (128 // hd) for c in range(feat // 128)]

    def peers(part, k):
        return [pltpu.make_async_remote_copy(src_ref=part.at[0], dst_ref=part.at[j], send_sem=part_send.at[k, j], recv_sem=part_recv.at[k, j],
                                             device_id={"sp": peer}, device_id_type=MESH) for j, peer in ((1, partner), (2, cross), (3, diag))]

    def share(part, k, base):
        for b in range(part.shape[1]):
            part[0, b:b + 1, :] = rows_acc[base + b]
        for copy in peers(part, k):
            copy.start()

    def exchange(send, recv, k):
        return pltpu.make_async_remote_copy(src_ref=send, dst_ref=recv, send_sem=att_sem.at[k, 0], recv_sem=att_sem.at[k, 1],
                                            device_id={"tp": 1 - tp}, device_id_type=MESH)

    def merge(part, k):
        for copy in peers(part, k):
            copy.wait()
        blocks = []
        for s in range(4):
            j = lax.rem(chip + s // 2, 2) * 2 + lax.rem(core + s % 2, 2)
            blocks.append(part[j])
        tops = [x[:, feat:] for x in blocks]
        top_all = functools.reduce(jnp.maximum, tops)
        scale = [jnp.exp(t - top_all) for t in tops]
        total = sum(s * pltpu.roll(t, 128 - nh, axis=1) for s, t in zip(scale, tops))
        context = jnp.zeros((part.shape[1], feat), F32)
        for s, x in zip(scale, blocks):
            factor = s / total
            wide = jnp.concatenate([sum(jnp.where(lane_heads[c][:1] == h, factor[:, h:h + 1], 0.0) for h in range(c * (128 // hd), (c + 1) * (128 // hd))) for c in range(feat // 128)], axis=1)
            context = context + wide * x[:, :feat]
        return jnp.dot(context.astype(BF16), wo[...], preferred_element_type=F32)

    def finish_early():
        wo_copy.wait()
        asend_e[...] = merge(part_e, 0)
        exchange(asend_e, arecv_e, 0).start()

    for g in range(stages):
        late = rel_cro[g + 1].shape[0] if g + 1 < stages else 0
        first_step = max(g * group - 1, 0)
        last_step = g * group + group - 2
        if g > 0:
            settle(g)
        for c in range(late - (last_step - first_step + 1)):
            arrive(g + 1, c)

        @pl.loop(first_step, last_step + 1)
        def _(i):
            if late:
                arrive(g + 1, i - last_step + late - 1)

            if g == stages - 1:
                @pl.when(i == nb - LATE)
                def _():
                    share(part_e, 0, 0)

            v_load(i).wait()
            mix(i, lax.rem(i, 2))
            score(g, i + 1, lax.rem(i + 1, 2))

            if first_step < nb - NS:
                @pl.when(i < nb - NS)
                def _():
                    v_load(i + NS).start()

    wu_copy.start()
    wd_copy.start()
    v_load(nb - 1).wait()
    mix(nb - 1, (nb - 1) % 2)

    def down_copies(send, recv, k):
        return [pltpu.make_async_remote_copy(src_ref=send.at[c], dst_ref=recv.at[c], send_sem=ex_send.at[k, c], recv_sem=ex_recv.at[k, c],
                                             device_id={"tp": 1 - tp}, device_id_type=MESH) for c in range(send.shape[0])]

    def mlp(rows, attn, send, recv, k):
        middle = (rows + attn).astype(BF16).astype(F32)
        normed_mlp = rms(middle, gm_ref[...][None].astype(F32))
        up = jnp.dot(normed_mlp, wu[...], preferred_element_type=F32)
        act = jax.nn.gelu(up, approximate=True).astype(BF16)
        cols = send.shape[2]
        for c, copy in enumerate(down_copies(send, recv, k)):
            send[c] = jnp.dot(act, wd[:, c * cols:(c + 1) * cols], preferred_element_type=F32)
            copy.start()
        return middle

    def finish(middle, send, recv, k):
        done = []
        cols = send.shape[2]
        for c, copy in enumerate(down_copies(send, recv, k)):
            copy.wait()
            done.append(middle[:, c * cols:(c + 1) * cols] + (send[c] + recv[c]))
        return jnp.concatenate(done, axis=1)

    cut = nb - LATE
    share(part_l, 1, cut)
    finish_early()
    asend_l[...] = merge(part_l, 1)
    exchange(asend_l, arecv_l, 1).start()
    exchange(asend_e, arecv_e, 0).wait()
    wu_copy.wait()
    wd_copy.wait()
    middle_e = mlp(hidden[:cut], asend_e[...] + arecv_e[...], dsend_e, drecv_e, 0)
    exchange(asend_l, arecv_l, 1).wait()
    middle_l = mlp(hidden[cut:], asend_l[...] + arecv_l[...], dsend_l, drecv_l, 1)
    first = finish(middle_e, dsend_e, drecv_e, 0)
    last = finish(middle_l, dsend_l, drecv_l, 1)
    out_ref[...] = jnp.concatenate([first, last], axis=0).astype(BF16)


def solution(mesh):
    spec_cache = P('dp', 'sp', 'tp', None)
    in_specs = (P('dp', None), spec_cache, spec_cache, P('dp'), P('sp', 'tp', None), P('tp', None), P('tp', None), P(None), P(None, 'tp', None), P(None, 'tp', None), P(None, 'tp', None), P('tp', None, None), P(None), P(None, 'tp'), P('tp', None))

    def layer_step(hidden, k_cache, v_cache, lengths, rel_table, u_bias, w_bias, g_attn, w_query, w_key, w_value, w_out, g_mlp, w_up, w_down):
        nb, width, nh, hd = k_cache.shape
        feat = nh * hd
        model = hidden.shape[1]
        k_t = k_cache.transpose(0, 2, 3, 1).reshape(nb, feat, width)
        v_t = v_cache.transpose(0, 2, 3, 1).reshape(nb, feat, width)
        r_t = rel_table.transpose(1, 2, 0).reshape(feat, width)
        proj = [w.transpose(1, 2, 0).reshape(feat, model) for w in (w_query, w_key, w_value)]
        vmem = pl.BlockSpec(memory_space=pltpu.VMEM)
        hbm = pl.BlockSpec(memory_space=pl.ANY)
        smem = pl.BlockSpec(memory_space=pltpu.SMEM)
        large = 1, 2, 4, 8, 9, 10, 11, 13, 14
        dma = pltpu.SemaphoreType.DMA
        full = 2 * ((0, nb),)
        tight = (0, 4, 7, 10, 13), (0, 3, 5, 7, 8)

        def call(caps, *operands):
            compact = caps != full
            rows = caps[0][-1]
            return pl.pallas_call(
                functools.partial(kernel, caps),
                out_shape=(jax.ShapeDtypeStruct((nb, model), BF16), jax.ShapeDtypeStruct((1,), jnp.int32)),
                in_specs=[hbm if compact or i in large else smem if i == 3 else vmem for i in range(15)],
                out_specs=(vmem, pl.BlockSpec(memory_space=pltpu.SMEM)),
                scratch_shapes=[
                    pltpu.VMEM(hidden.shape, BF16),
                    pltpu.SMEM(lengths.shape, jnp.int32),
                    pltpu.VMEM(u_bias.shape, BF16),
                    pltpu.VMEM(w_bias.shape, BF16),
                    pltpu.VMEM(g_attn.shape, BF16),
                    pltpu.VMEM(g_mlp.shape, BF16),
                    pltpu.VMEM((NS, feat, width), BF16),
                    pltpu.VMEM((nb, nh, width), F32),
                    pltpu.VMEM((nb, nh, width), F32),
                    pltpu.VMEM((nb, nh, width), F32),
                    pltpu.VMEM((2, nh, width), BF16),
                    pltpu.VMEM((2, nh, 128), F32),
                    pltpu.VMEM((feat, model), BF16),
                    pltpu.VMEM(w_up.shape, BF16),
                    pltpu.VMEM(w_down.shape, BF16),
                    pltpu.VMEM((nb, 16, feat), BF16),
                    pltpu.VMEM((nb, feat), F32),
                    pltpu.VMEM((nb, feat), F32),
                    pltpu.VMEM((nb, 1, feat + 128), F32),
                    pltpu.VMEM((4, nb - LATE, feat + 128), F32),
                    pltpu.VMEM((4, LATE, feat + 128), F32),
                    pltpu.VMEM((nb - LATE, model), F32),
                    pltpu.VMEM((nb - LATE, model), F32),
                    pltpu.VMEM((LATE, model), F32),
                    pltpu.VMEM((LATE, model), F32),
                    pltpu.VMEM((2, nb - LATE, model // 2), F32),
                    pltpu.VMEM((2, nb - LATE, model // 2), F32),
                    pltpu.VMEM((2, LATE, model // 2), F32),
                    pltpu.VMEM((2, LATE, model // 2), F32),
                    dma((NS,)), dma((12,)), dma((4,)), dma((2,)), dma((rows,)), dma((rows,)), dma((rows,)), dma((rows,)), dma((2, 4)), dma((2, 4)), dma((2, 2)), dma((2, 2)), dma((2, 2)),
                    pltpu.SMEM((2, nb), jnp.int32),
                ] + 2 * [pltpu.VMEM((b - a, nh, width), F32) for a, b in zip(caps[0], caps[0][1:])] + ([pltpu.VMEM((rows, nh, width), F32)] if compact else []),
                compiler_params=pltpu.CompilerParams(collective_id=int(compact), has_side_effects=True, vmem_limit_bytes=(57 if compact else 63) * 2 ** 20),
            )(*operands)

        operands = (hidden, k_t, v_t, lengths, r_t, u_bias, w_bias, g_attn, *proj, w_out.reshape(feat, model), g_mlp, w_up, w_down)
        out, fits = call(tight, *operands)
        return lax.cond(fits[0] > 0, lambda *_: out, lambda *full_operands: call(full, *full_operands)[0], *operands)

    return jax.shard_map(layer_step, mesh=mesh, in_specs=in_specs, out_specs=P('dp', None), check_vma=False)
```
